16 devices in a mesh: rep: 2 (over y, z), dp: 8 (over x, core).
Axes of the slice: x: 4, y: 2, z: 1, core: 2. Of those that a mesh axis runs over, the one named last changes fastest.
The devices are a block of a 4x4x8 slice.
Arguments:
- x: bfloat16 [16, 2048, 1024], P(('rep', 'dp')), parts along dimension 0
- dy: bfloat16 [16, 2048, 1024], P(('rep', 'dp')), parts along dimension 0
- w_gate: bfloat16 [2, 1024, 3328], replicated
- w_up: bfloat16 [2, 1024, 3328], replicated
- w_down: bfloat16 [2, 3328, 1024], replicated
- m_w_gate: float32 [2, 1024, 3328], P(None, 'dp')
- m_w_up: float32 [2, 1024, 3328], P(None, 'dp')
- m_w_down: float32 [2, 3328, 1024], P(None, 'dp')
- v_w_gate: float32 [2, 1024, 3328], P(None, 'dp')
- v_w_up: float32 [2, 1024, 3328], P(None, 'dp')
- v_w_down: float32 [2, 3328, 1024], P(None, 'dp')
Outputs:
- output 1: bfloat16 [4, 1024, 3328], P('rep'), parts along dimension 0
- output 2: bfloat16 [4, 1024, 3328], P('rep'), parts along dimension 0
- output 3: bfloat16 [4, 3328, 1024], P('rep'), parts along dimension 0
- output 4: float32 [4, 1024, 3328], P('rep', 'dp'), parts along dimension 0
- output 5: float32 [4, 1024, 3328], P('rep', 'dp'), parts along dimension 0
- output 6: float32 [4, 3328, 1024], P('rep', 'dp'), parts along dimension 0
- output 7: float32 [4, 1024, 3328], P('rep', 'dp'), parts along dimension 0
- output 8: float32 [4, 1024, 3328], P('rep', 'dp'), parts along dimension 0
- output 9: float32 [4, 3328, 1024], P('rep', 'dp'), parts along dimension 0
There are 2 independent parts. The reference program is written for one: setup_inputs(seed, part) draws one part's arguments, and reference() takes and returns one part's arrays. A program takes and returns all parts, laid end to end along the dimension named above; an argument that names none is the same for every part.
All inputs are finite; a program needn't handle non-finite values.
Results may differ from the reference program's by a relative error of at most 0.022.
Values are sent between devices in bfloat16 or wider.
A program may use at most 768 MiB of HBM per device.

```python
import jax
import jax.numpy as jnp
from jax import lax

SEQUENCES = 8
TOKENS = 2048
D = 1024
FF = 3328
LAYERS = 2
NAMES = ("w_gate", "w_up", "w_down")
SHAPES = {"w_gate": (LAYERS, D, FF), "w_up": (LAYERS, D, FF), "w_down": (LAYERS, FF, D)}


def bump(key, n, height):
    away = (jnp.arange(n, dtype=jnp.int32) - jax.random.randint(key, (), 0, n, jnp.int32)) % n
    return jnp.where(away < n // 8, height, 1.0)


def together(key, own, strength):
    shared = jax.random.normal(key, own.shape[1:], jnp.float32)
    return (own + strength * shared) * lax.rsqrt(1 + strength * strength)


def setup_inputs(seed: int = 0, part: int = 0) -> dict:
    kx, kdy, ka, kb, kz, kf, kh, kl, *keys = jax.random.split(jax.random.key(seed), 8 + 3 * len(NAMES))
    kx, kdy, ka, kb = (jax.random.fold_in(k, part) for k in (kx, kdy, ka, kb))
    kw, km, kv = (keys[i::3] for i in range(3))
    shape = (SEQUENCES, TOKENS, D)
    much_x, much_dy = jax.random.uniform(kz, (2,), jnp.float32, 0.0, 1.0)
    loud = 2.0 ** jax.random.uniform(jax.random.fold_in(kz, 1), (), jnp.float32, -1.0, 2.0)
    layers = 2.0 ** jax.random.uniform(kl, (LAYERS, 1, 1), jnp.float32, -1.0, 1.0)
    x = together(ka, jax.random.normal(kx, shape, jnp.float32), much_x) * bump(kf, D, 4.0)
    dy = together(kb, jax.random.normal(kdy, shape, jnp.float32), much_dy)
    drawn = {"x": x.astype(jnp.bfloat16), "dy": (loud * dy * (SEQUENCES * TOKENS) ** -0.5).astype(jnp.bfloat16)}
    for key, name in zip(kw, NAMES, strict=True):
        w = jax.random.normal(key, SHAPES[name], jnp.float32) * SHAPES[name][1] ** -0.5
        drawn[name] = (w * {"w_gate": 1.0, "w_up": bump(kh, FF, 4.0), "w_down": layers}[name]).astype(jnp.bfloat16)
    for key, name in zip(km, NAMES, strict=True):
        drawn[f"m_{name}"] = 0.1 * jax.random.normal(key, SHAPES[name], jnp.float32)
    for key, name in zip(kv, NAMES, strict=True):
        drawn[f"v_{name}"] = jax.random.uniform(key, SHAPES[name], jnp.float32, 0.005, 0.015)
    return drawn


def matmul(a, w):
    return jnp.dot(a, w, preferred_element_type=jnp.float32).astype(jnp.bfloat16)


def normed(h):
    wide = h.astype(jnp.float32)
    scale = lax.rsqrt(jnp.mean(wide**2, -1, keepdims=True) + 1e-6)
    return (wide * scale).astype(jnp.bfloat16)


def layer(h, w):
    a = normed(h)
    gate = jnp.dot(a, w["w_gate"], preferred_element_type=jnp.float32)
    up = jnp.dot(a, w["w_up"], preferred_element_type=jnp.float32)
    return h + matmul((jax.nn.silu(gate) * up).astype(jnp.bfloat16), w["w_down"])


def adamw(w, m, v, g):
    m = 0.9 * m + 0.1 * g
    v = 0.95 * v + 0.05 * g * g
    step = m * lax.rsqrt(v + 1e-8) + 0.1 * w
    return (w - 0.02 * step).astype(jnp.bfloat16), m, v


def stack(weights, h):
    return lax.scan(lambda h, w: (layer(h, w), None), h, weights)[0]


def reference(x, dy, w_gate, w_up, w_down, m_w_gate, m_w_up, m_w_down, v_w_gate, v_w_up, v_w_down):
    weights = dict(zip(NAMES, (w_gate, w_up, w_down), strict=True))

    def take(so_far, sequence):
        h, by_y = sequence
        _, back = jax.vjp(lambda w: stack(w, h), weights)
        return jax.tree.map(lambda total, term: total + term.astype(jnp.float32), so_far, back(by_y)[0]), None

    none_yet = {name: jnp.zeros(w.shape, jnp.float32) for name, w in weights.items()}
    by_weights, _ = lax.scan(take, none_yet, (x, dy))
    gradients = [by_weights[name].astype(jnp.bfloat16).astype(jnp.float32) for name in NAMES]
    new = [
        adamw(w.astype(jnp.float32), m, v, g)
        for w, m, v, g in zip((w_gate, w_up, w_down), (m_w_gate, m_w_up, m_w_down), (v_w_gate, v_w_up, v_w_down), gradients, strict=True)
    ]
    return tuple(one[which] for which in range(3) for one in new)
```

```python
import functools

import jax
import jax.numpy as jnp
from jax import lax
from jax.experimental import pallas as pl
from jax.experimental.pallas import tpu as pltpu
from jax.sharding import PartitionSpec as P

f32 = jnp.float32
bf16 = jnp.bfloat16
VMEM_LIMIT = 60 * 1024 * 1024
TN = 256


def params(**kw):
    return pltpu.CompilerParams(vmem_limit_bytes=VMEM_LIMIT, **kw)


def cost(flops, bytes_accessed):
    return pl.CostEstimate(flops=flops, bytes_accessed=bytes_accessed, transcendentals=0)


def sds(shape, dtype):
    return jax.ShapeDtypeStruct(shape, dtype)


NT = (((1,), (1,)), ((), ()))
TNN = (((0,), (0,)), ((), ()))


def mm(a, b):
    return jnp.dot(a, b, preferred_element_type=f32)


def fwd_kernel(rows, x_ref, wg_ref, wu_ref, a_ref, act_ref, gate_ref, up_ref):
    t = x_ref.shape[0]

    @pl.when(pl.program_id(0) == 0)
    def _():
        for r in range(0, t, rows):
            wide = x_ref[r : r + rows, :].astype(f32)
            scale = lax.rsqrt(jnp.mean(wide * wide, -1, keepdims=True) + 1e-6)
            a_ref[r : r + rows, :] = (wide * scale).astype(bf16)

    for r in range(0, t, rows):
        a = a_ref[r : r + rows, :]
        g = mm(a, wg_ref[...])
        u = mm(a, wu_ref[...])
        gate_ref[r : r + rows, :] = g
        up_ref[r : r + rows, :] = u
        act_ref[r : r + rows, :] = (g * jax.nn.sigmoid(g) * u).astype(bf16)


def fwd(x, w_gate, w_up, l):
    t, d = x.shape
    f = w_gate.shape[2]
    whole = pl.BlockSpec((t, d), lambda j: (0, 0))
    wspec = pl.BlockSpec((None, d, TN), lambda j: (l, 0, j))
    tile = pl.BlockSpec((t, TN), lambda j: (0, j))
    return pl.pallas_call(
        functools.partial(fwd_kernel, 512),
        name=f"fwd_gate_up_{l}",
        grid=(f // TN,),
        in_specs=[whole, wspec, wspec],
        out_specs=[whole, tile, tile, tile],
        out_shape=[sds((t, d), bf16), sds((t, f), bf16), sds((t, f), f32), sds((t, f), f32)],
        compiler_params=params(),
        cost_estimate=cost(4 * t * d * f, 4 * d * f + 10 * t * f + 4 * t * d),
    )(x, w_gate, w_up)


def down_kernel(x_ref, act_ref, w_ref, h_ref, a_ref):
    y = mm(act_ref[...], w_ref[...]).astype(bf16)
    h = (x_ref[...].astype(f32) + y.astype(f32)).astype(bf16)
    h_ref[...] = h
    wide = h.astype(f32)
    scale = lax.rsqrt(jnp.mean(wide * wide, -1, keepdims=True) + 1e-6)
    a_ref[...] = (wide * scale).astype(bf16)


def down(x, act, w_down, l):
    t, d = x.shape
    f = act.shape[1]
    tm = 256
    row = pl.BlockSpec((tm, d), lambda i: (i, 0))
    return pl.pallas_call(
        down_kernel,
        name=f"down_{l}",
        grid=(t // tm,),
        in_specs=[row, pl.BlockSpec((tm, f), lambda i: (i, 0)), pl.BlockSpec((None, f, d), lambda i: (l, 0, 0))],
        out_specs=[row, row],
        out_shape=[sds((t, d), bf16), sds((t, d), bf16)],
        compiler_params=params(),
        cost_estimate=cost(2 * t * d * f, 2 * d * f + 2 * t * f + 6 * t * d),
    )(x, act, w_down)


def silu_back(g, u, dact):
    s = jax.nn.sigmoid(g)
    gs = g * s
    dgate = dact * u * (s + gs * (1.0 - s))
    return dgate.astype(bf16), (dact * gs).astype(bf16)


def grads_kernel(chips, tiles, keeps, *refs):
    a_ref, dy_ref, p_ref, q_ref, wd_ref = refs[:5]
    refs = refs[5:]
    if keeps:
        (down_ref, g_ref), (dg_ref, du_ref), refs = refs[:2], refs[2:4], refs[4:]
    else:
        (dg_ref, du_ref, down_ref, g_ref), refs = refs[:4], refs[4:]
    at_ref, act_ref, out, keep, got, across, near, own, from_near, from_far, psem, sem1, sem2 = refs
    t, d = a_ref.shape
    r = d // (2 * chips)
    half = r // 2
    me = lax.axis_index("dp")
    n = 2 * chips
    chip, core = me // 2, lax.rem(me, 2)
    partner = chip * 2 + 1 - core
    sides = (lax.rem(me + 2, n), lax.rem(me + n - 2, n))
    step = pl.program_id(0)

    def remote(src, dst, sems, slot, to):
        return pltpu.make_async_remote_copy(
            src_ref=src,
            dst_ref=dst,
            send_sem=sems.at[0, slot],
            recv_sem=sems.at[1, slot],
            device_id={"dp": to},
            device_id_type=pl.DeviceIdType.MESH,
        )

    def pair_copy(slot):
        return remote(out.at[slot], got.at[slot], psem, slot, partner)

    def first_copy(slot, side):
        return remote(across.at[slot, side], from_far.at[slot, side], sem1.at[side], slot, sides[side])

    def second_copy(slot, side):
        return remote(near.at[slot, side], from_near.at[slot, side], sem2.at[side], slot, sides[side])

    @pl.when(step == 0)
    def _():
        barrier = pltpu.get_barrier_semaphore()
        for to in (partner, *sides):
            pl.semaphore_signal(barrier, inc=1, device_id={"dp": to}, device_id_type=pl.DeviceIdType.MESH)
        for part, which in enumerate((1 - core, core)):
            for x in range(chips):
                at = pl.multiple_of((2 * x + which) * r, 128)
                to = (part * chips + x) * r
                at_ref[to : to + r, :] = a_ref[:, pl.ds(at, r)].T
        pl.semaphore_wait(barrier, 3)

    @pl.when(step < tiles)
    def _():
        slot = lax.rem(step, 2)
        rows = 512
        for lo in range(0, t, rows):
            at = slice(lo, lo + rows)
            if keeps:
                g, u = p_ref[at, :], q_ref[at, :]
            else:
                g, u = mm(a_ref[at, :], p_ref[...]), mm(a_ref[at, :], q_ref[...])
            dact = lax.dot_general(dy_ref[at, :], wd_ref[...], NT, preferred_element_type=f32)
            act_ref[at, :] = (g * jax.nn.sigmoid(g) * u).astype(bf16)
            dg_ref[at, :], du_ref[at, :] = silu_back(g, u, dact.astype(bf16).astype(f32))
        for s, ref in enumerate((dg_ref, du_ref)):
            for half_, to in ((0, out), (1, keep)):
                term = mm(at_ref[half_ * (d // 2) : (half_ + 1) * (d // 2), :], ref[...]).astype(bf16)
                for x in range(chips):
                    to[slot, x, s] = term[x * r : (x + 1) * r]
        down_ref[...] = lax.dot_general(act_ref[...], dy_ref[...], TNN, preferred_element_type=f32).astype(bf16)

    def add(x, y):
        return (x.astype(f32) + y.astype(f32)).astype(bf16)

    @pl.when((step >= 3) & (step < tiles + 3))
    def _():
        slot = lax.rem(step + 1, 2)
        for side in range(2):
            second_copy(slot, side).wait()
        total = own[slot].astype(f32) + from_near[slot, 0].astype(f32) + from_near[slot, 1].astype(f32)
        g_ref[...] = total.astype(bf16)

    @pl.when((step >= 2) & (step < tiles + 2))
    def _():
        slot = lax.rem(step, 2)
        for side in range(2):
            first_copy(slot, side).wait()
        near[slot, 0, :, :half] = add(near[slot, 0, :, :half], from_far[slot, 0])
        near[slot, 1, :, half:] = add(near[slot, 1, :, half:], from_far[slot, 1])

    @pl.when((step >= 1) & (step < tiles + 1))
    def _():
        slot = lax.rem(step + 1, 2)
        pair_copy(slot).wait()

        def total(hop):
            i = lax.rem(chip + hop, chips)
            return add(keep[slot, i], got[slot, i])

        far = total(chips // 2)
        across[slot, 0] = far[:, :half]
        across[slot, 1] = far[:, half:]
        near[slot, 0] = total(1)
        near[slot, 1] = total(chips - 1)
        own[slot] = total(0)

    @pl.when((step >= 2) & (step < tiles + 2))
    def _():
        for side in range(2):
            second_copy(lax.rem(step, 2), side).start()

    @pl.when((step >= 1) & (step < tiles + 1))
    def _():
        for side in range(2):
            first_copy(lax.rem(step + 1, 2), side).start()

    @pl.when(step < tiles)
    def _():
        pair_copy(lax.rem(step, 2)).start()


def grads(a, dy, p, q, w_down, l, chips, keeps, name):
    t, d = a.shape
    f = w_down.shape[1]
    tiles = f // TN
    r = d // (2 * chips)
    whole = pl.BlockSpec((t, d), lambda j: (0, 0))

    def at(j):
        return jnp.minimum(j, tiles - 1)

    tile = pl.BlockSpec((t, TN), lambda j: (0, at(j)))
    wspec = tile if keeps else pl.BlockSpec((None, d, TN), lambda j: (l, 0, at(j)))
    dspec = pl.BlockSpec((None, TN, d), lambda j: (l, at(j), 0))
    out_specs = [pl.BlockSpec((TN, d), lambda j: (at(j), 0)), pl.BlockSpec((2, r, TN), lambda j: (0, 0, jnp.maximum(j - 3, 0)))]
    out_shape = [sds((f, d), bf16), sds((2, r, f), bf16)]
    scratch = [pltpu.VMEM((t, TN), bf16)] * 2
    if not keeps:
        out_specs, out_shape, scratch = [tile, tile] + out_specs, [sds((t, f), bf16)] * 2 + out_shape, []
    dma = pltpu.SemaphoreType.DMA
    scratch += [
        pltpu.VMEM((d, t), bf16),
        pltpu.VMEM((t, TN), bf16),
        pltpu.VMEM((2, chips, 2, r, TN), bf16),
        pltpu.VMEM((2, chips, 2, r, TN), bf16),
        pltpu.VMEM((2, chips, 2, r, TN), bf16),
        pltpu.VMEM((2, 2, 2, r // 2, TN), bf16),
        pltpu.VMEM((2, 2, 2, r, TN), bf16),
        pltpu.VMEM((2, 2, r, TN), bf16),
        pltpu.VMEM((2, 2, 2, r, TN), bf16),
        pltpu.VMEM((2, 2, 2, r // 2, TN), bf16),
        dma((2, 2)),
        dma((2, 2, 2)),
        dma((2, 2, 2)),
    ]
    mms = 4 if keeps else 6
    return pl.pallas_call(
        functools.partial(grads_kernel, chips, tiles, keeps),
        name=f"grads_{name}",
        grid=(tiles + 3,),
        in_specs=[whole, whole, wspec, wspec, dspec],
        out_specs=out_specs,
        out_shape=out_shape,
        scratch_shapes=scratch,
        compiler_params=params(collective_id=l, has_side_effects=True),
        cost_estimate=cost(2 * mms * t * d * f, 20 * t * f),
    )(a, dy, p, q, w_down)


def dh_kernel(cuts, *refs):
    n = len(cuts)
    dgs, dus, (wg_ref, wu_ref, h_ref, dy_ref, out_ref) = refs[:n], refs[n : 2 * n], refs[2 * n :]
    da = None
    for dg, du, (lo, hi) in zip(dgs, dus, cuts):
        for g, w in ((dg, wg_ref), (du, wu_ref)):
            term = lax.dot_general(g[...], w[:, lo:hi], NT, preferred_element_type=f32)
            da = term if da is None else da + term
    da = da.astype(bf16).astype(f32)
    wide = h_ref[...].astype(f32)
    scale = lax.rsqrt(jnp.mean(wide * wide, -1, keepdims=True) + 1e-6)
    norm = wide * scale
    back_ = scale * (da - norm * jnp.mean(da * norm, -1, keepdims=True))
    out_ref[...] = (dy_ref[...].astype(f32) + back_.astype(bf16).astype(f32)).astype(bf16)


def dh(dgs, dus, w_gate, w_up, h, dy, l):
    t, d = h.shape
    f = w_gate.shape[2]
    tm = 256
    cuts, at = [], 0
    for g in dgs:
        cuts.append((at, at + g.shape[1]))
        at += g.shape[1]
    row = pl.BlockSpec((tm, d), lambda i: (i, 0))
    chunks = [pl.BlockSpec((tm, g.shape[1]), lambda i: (i, 0)) for g in dgs]
    wspec = pl.BlockSpec((None, d, f), lambda i: (l, 0, 0))
    return pl.pallas_call(
        functools.partial(dh_kernel, tuple(cuts)),
        name=f"grad_input_{l}",
        grid=(t // tm,),
        in_specs=chunks + chunks + [wspec, wspec, row, row],
        out_specs=row,
        out_shape=sds((t, d), bf16),
        compiler_params=params(),
        cost_estimate=cost(4 * t * d * f, 4 * d * f + 4 * t * f + 6 * t * d),
    )(*dgs, *dus, w_gate, w_up, h, dy)


def width(c):
    return c // 2 if c % 256 == 0 else c


def pair_kernel(chips, got_ref, keep_ref, across_a, across_b, right, left, own):
    me = lax.axis_index("dp")
    chip, core = me // 2, lax.rem(me, 2)
    half = got_ref.shape[1] // 2

    def total(hop):
        i = lax.rem(chip + hop, chips)
        mine = keep_ref[i, core] if len(keep_ref.shape) == 4 else keep_ref[i]
        return (mine.astype(f32) + got_ref[i].astype(f32)).astype(bf16)

    across = total(2)
    across_a[...] = across[:half]
    across_b[...] = across[half:]
    right[...] = total(1)
    left[...] = total(3)
    own[...] = total(0)


def pair_add(got, keep, name):
    s, chips, r, c = got.shape
    tc = width(c)
    whole = pl.BlockSpec((None, chips, r, tc), lambda i, j: (i, 0, 0, j))
    wide = pl.BlockSpec((None, chips, 2, r, tc), lambda i, j: (i, 0, 0, 0, j)) if keep.ndim == 5 else whole
    one = pl.BlockSpec((None, r, tc), lambda i, j: (i, 0, j))
    half = pl.BlockSpec((None, r // 2, tc), lambda i, j: (i, 0, j))
    return pl.pallas_call(
        functools.partial(pair_kernel, chips),
        name=f"pair_add_{name}",
        grid=(s, c // tc),
        in_specs=[whole, wide],
        out_specs=[half, half, one, one, one],
        out_shape=[sds((s, r // 2, c), bf16)] * 2 + [sds((s, r, c), bf16)] * 3,
        compiler_params=params(),
        cost_estimate=cost(16 * s * r * c, 24 * s * r * c),
    )(got, keep)


def fold_kernel(right, left, a, b, right_out, left_out):
    right_out[...] = (right[...].astype(f32) + a[...].astype(f32)).astype(bf16)
    left_out[...] = (left[...].astype(f32) + b[...].astype(f32)).astype(bf16)


def fold(right, left, a, b, name):
    s, r, c = right.shape
    tc = width(c)
    lo = pl.BlockSpec((None, r // 2, tc), lambda i, j: (i, 0, j))
    hi = pl.BlockSpec((None, r // 2, tc), lambda i, j: (i, 1, j))
    return pl.pallas_call(
        fold_kernel,
        name=f"fold_{name}",
        grid=(s, c // tc),
        in_specs=[lo, hi, lo, lo],
        out_specs=[lo, hi],
        out_shape=[sds((s, r, c), bf16)] * 2,
        input_output_aliases={0: 0, 1: 1},
        compiler_params=params(),
        cost_estimate=cost(4 * s * r * c, 6 * s * r * c),
    )(right, left, a, b)


def adamw_kernel(n, *refs):
    sums, (w_ref, m_ref, v_ref), (nw_ref, nm_ref, nv_ref) = refs[:n], refs[n : n + 3], refs[-3:]
    g = sums[0][...].astype(f32)
    for other in sums[1:]:
        g = g + other[...].astype(f32)
    g = g.astype(bf16).astype(f32)
    m = 0.9 * m_ref[...] + 0.1 * g
    v = 0.95 * v_ref[...] + 0.05 * g * g
    w = w_ref[...].astype(f32)
    nm_ref[...] = m
    nv_ref[...] = v
    nw_ref[...] = (w - 0.02 * (m * lax.rsqrt(v + 1e-8) + 0.1 * w)).astype(bf16)


def adamw(sums, s, w, m, v, l, col, moments, new, name):
    n, r, c = sums[0].shape
    tr, tc = r // 2, TN if col or c < m.shape[2] else width(c)
    part = pl.BlockSpec((None, tr, tc), lambda i, j: (s, i, j))
    block = pl.BlockSpec((None, tr, tc), lambda i, j: (l, i, j + col // tc))
    anyspec = pl.BlockSpec(memory_space=pl.ANY)
    more, alias = [], {}
    for at, t in ((0, new),) + ((1, None), (2, None)) if moments is None else ((0, new), (1, moments[0]), (2, moments[1])):
        if t is not None:
            alias[len(sums) + 3 + len(more)] = at
            more.append(t)
    return pl.pallas_call(
        functools.partial(adamw_kernel, len(sums)),
        name=f"adamw_{name}",
        grid=(r // tr, c // tc),
        in_specs=[part] * len(sums) + [block] * 3 + [anyspec] * len(more),
        out_specs=[part, block, block],
        out_shape=[sds((n, r, c), bf16), sds(m.shape, f32), sds(v.shape, f32)],
        input_output_aliases=alias,
        compiler_params=params(),
        cost_estimate=cost(20 * r * c, 30 * r * c),
    )(*sums, w, m, v, *more)


def place_kernel(l, col, chips, kinds, n, k, *refs):
    pieces = refs[:n]
    refs = refs[n:]
    bufs, (isem, osem) = refs[-n - 2 : -2], refs[-2:]
    outs = refs[-n - 2 - k : -n - 2]
    me = lax.axis_index("dp")
    x, core = me // 2, lax.rem(me, 2)
    ins = []
    for i in range(n):
        cp = pltpu.make_async_copy(pieces[i], bufs[i], isem.at[i])
        cp.start()
        ins.append(cp)
    going = []
    for i, (hop, other, lo, hi) in enumerate(kinds):
        ins[i].wait()
        xi = lax.rem(x + hop, chips)
        ci = 1 - core if other else core
        for s, out in enumerate(outs):
            dst = out.at[l, xi, ci, pl.ds(lo, hi - lo), pl.ds(col, pieces[i].shape[2])]
            cp = pltpu.make_async_copy(bufs[i].at[s], dst, osem.at[i, s])
            cp.start()
            going.append(cp)
    for cp in going:
        cp.wait()


def place(pieces, kinds, shapes, l, col, into, chips, name):
    n, k = len(pieces), len(shapes)
    into = [t for t in into if t is not None]
    anyspec = pl.BlockSpec(memory_space=pl.ANY)
    moved = sum(p.size for p in pieces)
    return pl.pallas_call(
        functools.partial(place_kernel, l, col, chips, tuple(kinds), n, k),
        name=f"place_{name}",
        in_specs=[anyspec] * (n + len(into)),
        out_specs=[anyspec] * k,
        out_shape=[sds(shape, bf16) for shape in shapes],
        scratch_shapes=[pltpu.VMEM(p.shape, bf16) for p in pieces] + [pltpu.SemaphoreType.DMA((n,)), pltpu.SemaphoreType.DMA((n, k))],
        input_output_aliases={n + i: i for i in range(len(into))},
        compiler_params=params(),
        cost_estimate=cost(moved, 4 * moved),
    )(*pieces, *into)


def solution(mesh):
    n = mesh.shape["dp"]
    chips = n // 2
    PAIR = [(i, i ^ 1) for i in range(n)]
    RIGHT = [(i, (i + 2) % n) for i in range(n)]
    LEFT = [(i, (i - 2) % n) for i in range(n)]

    def send(t, way):
        return lax.ppermute(t, "dp", way)

    def body(x, dy, w_gate, w_up, w_down, m_gate, m_up, m_down, v_gate, v_up, v_down):
        me = lax.axis_index("dp")
        core = me % 2
        x, dy = x[0], dy[0]
        layers, d, f = w_gate.shape
        tiles = f // TN

        def block_of(w):
            r = w.shape[1] // n
            return lax.dynamic_slice_in_dim(w, me * r, r, 1)

        own_w = {"gate": block_of(w_gate), "up": block_of(w_up), "down": block_of(w_down)}
        m_in = {"gate": m_gate, "up": m_up, "down": m_down}
        v_in = {"gate": v_gate, "up": v_up, "down": v_down}
        moments, new_w = {}, {}

        class Unit:
            def __init__(self, keys, l, col, name, out=None, keep=None, total=None):
                self.keep, self.keys, self.l, self.col, self.name = keep, keys, l, col, name
                self.stage = 0
                if total is None:
                    self.flight = [send(out, PAIR)]
                else:
                    self.own, self.flight, self.stage = total, [], 2
                    self.advance()

            def advance(self):
                getattr(self, ("reduce_1", "reduce_2", "step", "gather_2", "gather_3", "finish")[self.stage])()
                self.stage += 1

            def reduce_1(self):
                a, b, self.right, self.left, self.own = pair_add(self.flight[0], self.keep, self.name)
                self.flight = [send(a, RIGHT), send(b, LEFT)]

            def reduce_2(self):
                right, left = fold(self.right, self.left, *self.flight, self.name)
                self.flight = [send(right, RIGHT), send(left, LEFT)]

            def step(self):
                w = None
                sums = [self.own, *self.flight]
                for s, key in enumerate(self.keys):
                    w, *moments[key] = adamw(
                        sums, s, own_w[key], m_in[key], v_in[key], self.l, self.col, moments.get(key), w, f"{self.name}_{key}"
                    )
                self.w = w
                self.flight = [send(w, RIGHT), send(w, LEFT), send(w, PAIR)]

            def gather_2(self):
                wl, wr, pw = self.flight
                half = wl.shape[1] // 2
                self.pieces = [self.w, wl, wr, pw]
                self.flight = [send(wl[:, :half], RIGHT), send(wr[:, half:], LEFT), send(wl, PAIR), send(wr, PAIR)]

            def gather_3(self):
                o1, o2, pwl, pwr = self.flight
                self.pieces += [pwl, pwr, o1, o2]
                self.flight = [send(o1, PAIR), send(o2, PAIR)]

            def finish(self):
                pieces = self.pieces + self.flight
                r = self.w.shape[1]
                half = r // 2
                kinds = [(0, False, 0, r), (3, False, 0, r), (1, False, 0, r), (0, True, 0, r), (3, True, 0, r), (1, True, 0, r)]
                kinds += [(2, o, lo, hi) for o in (False, True) for lo, hi in ((0, half), (half, r))]
                shapes = [(layers, chips, 2, r, own_w[key].shape[2]) for key in self.keys]
                into = [new_w.get(key) for key in self.keys]
                for key, t in zip(self.keys, place(pieces, kinds, shapes, self.l, self.col, into, chips, self.name)):
                    new_w[key] = t

        def after(units, *inputs):
            inputs, flights = lax.optimization_barrier((inputs, [u.flight for u in units]))
            for u, flight in zip(units, flights):
                u.flight = flight
                u.advance()
            return inputs

        def down_unit(g, l):
            g = g.reshape(1, chips, 2, f // n, d)
            out = lax.dynamic_index_in_dim(g, 1 - core, 2, keepdims=False)
            return Unit(("down",), l, 0, f"{l}d", out, g)

        kept = []
        h = x
        for l in range(layers - 1):
            a, act, gate, up = fwd(h, w_gate, w_up, l)
            kept.append((h, a, gate, up))
            h, a = down(h, act, w_down, l)
        l = layers - 1
        dg, du, g_down, total = grads(a, dy, w_gate, w_up, w_down, l, chips, False, f"{l}")
        pending = [down_unit(g_down, l), Unit(("gate", "up"), l, 0, f"{l}g", total=total)]
        for l in range(layers - 2, -1, -1):
            (dg, du) = after(pending[:1], dg, du)
            dy = dh([dg], [du], w_gate, w_up, h, dy, l + 1)
            h, a, gate, up = kept[l]
            (dy,) = after(pending, dy)
            g_down, total = grads(a, dy, gate, up, w_down, l, chips, True, f"{l}")
            g_down, total = after(pending, g_down, total)
            pending += [down_unit(g_down, l), Unit(("gate", "up"), l, 0, f"{l}g", total=total)]
        for u in pending:
            while u.stage < 6:
                u.advance()
        keys = ("gate", "up", "down")
        ws = tuple(new_w[k].reshape(w.shape) for k, w in zip(keys, (w_gate, w_up, w_down)))
        return ws + tuple(moments[k][0] for k in keys) + tuple(moments[k][1] for k in keys)

    seq, full, rows = P(("rep", "dp")), P(), P(None, "dp")
    out_m = P("rep", "dp")
    return jax.shard_map(
        body,
        mesh=mesh,
        in_specs=(seq, seq) + (full,) * 3 + (rows,) * 6,
        out_specs=(P("rep"),) * 3 + (out_m,) * 6,
        check_vma=False,
    )
```

```python
import functools

import jax
import jax.numpy as jnp
from jax import lax
from jax.experimental import pallas as pl
from jax.experimental.pallas import tpu as pltpu
from jax.sharding import PartitionSpec as P

f32 = jnp.float32
bf16 = jnp.bfloat16
VMEM_LIMIT = 60 * 1024 * 1024
TN = 256


def params(**kw):
    return pltpu.CompilerParams(vmem_limit_bytes=VMEM_LIMIT, **kw)


def cost(flops, bytes_accessed):
    return pl.CostEstimate(flops=flops, bytes_accessed=bytes_accessed, transcendentals=0)


def sds(shape, dtype):
    return jax.ShapeDtypeStruct(shape, dtype)


NT = (((1,), (1,)), ((), ()))
TNN = (((0,), (0,)), ((), ()))


def mm(a, b):
    return jnp.dot(a, b, preferred_element_type=f32)


def fwd_kernel(rows, x_ref, wg_ref, wu_ref, a_ref, act_ref):
    t = x_ref.shape[0]

    @pl.when(pl.program_id(0) == 0)
    def _():
        for r in range(0, t, rows):
            wide = x_ref[r : r + rows, :].astype(f32)
            scale = lax.rsqrt(jnp.mean(wide * wide, -1, keepdims=True) + 1e-6)
            a_ref[r : r + rows, :] = (wide * scale).astype(bf16)

    for r in range(0, t, rows):
        a = a_ref[r : r + rows, :]
        g = mm(a, wg_ref[...])
        u = mm(a, wu_ref[...])
        act_ref[r : r + rows, :] = (g * jax.nn.sigmoid(g) * u).astype(bf16)


def fwd(x, w_gate, w_up, l):
    t, d = x.shape
    f = w_gate.shape[2]
    whole = pl.BlockSpec((t, d), lambda j: (0, 0))
    wspec = pl.BlockSpec((None, d, TN), lambda j: (l, 0, j))
    tile = pl.BlockSpec((t, TN), lambda j: (0, j))
    return pl.pallas_call(
        functools.partial(fwd_kernel, 512),
        name=f"fwd_gate_up_{l}",
        grid=(f // TN,),
        in_specs=[whole, wspec, wspec],
        out_specs=[whole, tile],
        out_shape=[sds((t, d), bf16), sds((t, f), bf16)],
        compiler_params=params(),
        cost_estimate=cost(4 * t * d * f, 4 * d * f + 2 * t * f + 4 * t * d),
    )(x, w_gate, w_up)


def down_kernel(x_ref, act_ref, w_ref, h_ref, a_ref):
    y = mm(act_ref[...], w_ref[...]).astype(bf16)
    h = (x_ref[...].astype(f32) + y.astype(f32)).astype(bf16)
    h_ref[...] = h
    wide = h.astype(f32)
    scale = lax.rsqrt(jnp.mean(wide * wide, -1, keepdims=True) + 1e-6)
    a_ref[...] = (wide * scale).astype(bf16)


def down(x, act, w_down, l):
    t, d = x.shape
    f = act.shape[1]
    tm = 256
    row = pl.BlockSpec((tm, d), lambda i: (i, 0))
    return pl.pallas_call(
        down_kernel,
        name=f"down_{l}",
        grid=(t // tm,),
        in_specs=[row, pl.BlockSpec((tm, f), lambda i: (i, 0)), pl.BlockSpec((None, f, d), lambda i: (l, 0, 0))],
        out_specs=[row, row],
        out_shape=[sds((t, d), bf16), sds((t, d), bf16)],
        compiler_params=params(),
        cost_estimate=cost(2 * t * d * f, 2 * d * f + 2 * t * f + 6 * t * d),
    )(x, act, w_down)


def silu_back(g, u, dact):
    s = jax.nn.sigmoid(g)
    gs = g * s
    dgate = dact * u * (s + gs * (1.0 - s))
    return dgate.astype(bf16), (dact * gs).astype(bf16)


PAIRED, FOLDED, FINAL, SPREAD, ACROSS, DONE = 1, 2, 3, 4, 5, 6
SLOTS = 4


def grads_kernel(chips, tiles, wanted, *refs):
    a_ref, dy_ref, p_ref, q_ref, wd_ref = refs[:5]
    state = (refs[5:8], refs[8:11])
    refs = refs[11:]
    if wanted:
        (dg_ref, du_ref, down_ref, g_ref, full), refs = refs[:5], refs[5:]
    else:
        (down_ref, g_ref, full, dg_ref, du_ref), refs = refs[:5], refs[5:]
    at_ref, act_ref, out, keep, got, across, near, own, from_near, from_far, fresh, psem, sem1, sem2, gsem, lsem = refs
    t, d = a_ref.shape
    r = d // (2 * chips)
    half = r // 2
    me = lax.axis_index("dp")
    n = 2 * chips
    chip, core = me // 2, lax.rem(me, 2)
    partner = chip * 2 + 1 - core
    sides = (lax.rem(me + 2, n), lax.rem(me + n - 2, n))
    step = pl.program_id(0)

    def remote(src, dst, sems, slot, to):
        return pltpu.make_async_remote_copy(
            src_ref=src,
            dst_ref=dst,
            send_sem=sems.at[0, slot],
            recv_sem=sems.at[1, slot],
            device_id={"dp": to},
            device_id_type=pl.DeviceIdType.MESH,
        )

    def pair_copy(slot):
        return remote(out.at[slot], got.at[slot], psem, slot, partner)

    def first_copy(slot, side):
        return remote(across.at[slot, side], from_far.at[slot, side], sem1.at[side], slot, sides[side])

    def second_copy(slot, side):
        return remote(near.at[slot, side], from_near.at[slot, side], sem2.at[side], slot, sides[side])

    def place(x, at, lo=0, hi=r):
        return full.at[:, lax.rem(chip + x, chips), core, pl.ds(lo, hi - lo), pl.ds(pl.multiple_of(at * TN, TN), TN)]

    def gather_1(slot, at):
        here = place(0, at)
        ways = [remote(fresh.at[slot], here, gsem.at[i], slot, to) for i, to in enumerate((*sides, partner))]
        return [*ways, pltpu.make_async_copy(fresh.at[slot], here, lsem.at[slot])]

    def gather_2(slot, at):
        before, ahead = place(chips - 1, at), place(1, at)
        low, high = place(chips - 1, at, 0, half), place(1, at, half, r)
        ways = ((low, sides[0]), (high, sides[1]), (before, partner), (ahead, partner))
        return [remote(ref, ref, gsem.at[3 + i], slot, to) for i, (ref, to) in enumerate(ways)]

    def gather_3(slot, at):
        far = place(chips // 2, at)
        return [remote(far, far, gsem.at[7], slot, partner)]

    @pl.when(step == 0)
    def _():
        barrier = pltpu.get_barrier_semaphore()
        for to in (partner, *sides):
            pl.semaphore_signal(barrier, inc=1, device_id={"dp": to}, device_id_type=pl.DeviceIdType.MESH)
        for part, which in enumerate((1 - core, core)):
            for x in range(chips):
                at = pl.multiple_of((2 * x + which) * r, 128)
                to = (part * chips + x) * r
                at_ref[to : to + r, :] = a_ref[:, pl.ds(at, r)].T
        pl.semaphore_wait(barrier, 3)

    @pl.when(step < tiles)
    def _():
        rows = 512
        for lo in range(0, t, rows):
            at = slice(lo, lo + rows)
            g, u = mm(a_ref[at, :], p_ref[...]), mm(a_ref[at, :], q_ref[...])
            dact = lax.dot_general(dy_ref[at, :], wd_ref[...], NT, preferred_element_type=f32)
            act_ref[at, :] = (g * jax.nn.sigmoid(g) * u).astype(bf16)
            dg_ref[at, :], du_ref[at, :] = silu_back(g, u, dact.astype(bf16).astype(f32))

    def add(x, y):
        return (x.astype(f32) + y.astype(f32)).astype(bf16)

    def stage(lag):
        at = step - lag
        return (at >= 0) & (at < tiles), at, lax.rem(jnp.maximum(at, 0), SLOTS)

    on, _, slot = stage(FINAL)

    @pl.when(on)
    def _():
        for side in range(2):
            second_copy(slot, side).wait()
        total = own[slot].astype(f32) + from_near[slot, 0].astype(f32) + from_near[slot, 1].astype(f32)
        total = total.astype(bf16)
        g_ref[...] = total
        for i, (w_ref, m_ref, v_ref) in enumerate(state):
            g = total[i].astype(f32)
            m = 0.9 * m_ref[...] + 0.1 * g
            v = 0.95 * v_ref[...] + 0.05 * g * g
            w = w_ref[...].astype(f32)
            fresh[slot, i] = (w - 0.02 * (m * lax.rsqrt(v + 1e-8) + 0.1 * w)).astype(bf16)

    on, _, slot = stage(FOLDED)

    @pl.when(on)
    def _():
        for side in range(2):
            first_copy(slot, side).wait()
        near[slot, 0, :, :half] = add(near[slot, 0, :, :half], from_far[slot, 0])
        near[slot, 1, :, half:] = add(near[slot, 1, :, half:], from_far[slot, 1])

    on, at, slot = stage(PAIRED)

    @pl.when(on)
    def _():
        pair = lax.rem(at, 2)
        pair_copy(pair).wait()

        def total(hop):
            i = lax.rem(chip + hop, chips)
            return add(keep[pair, i], got[pair, i])

        far = total(chips // 2)
        across[slot, 0] = far[:, :half]
        across[slot, 1] = far[:, half:]
        near[slot, 0] = total(1)
        near[slot, 1] = total(chips - 1)
        own[slot] = total(0)

    def sides_of(copy):
        return lambda slot, at: [copy(slot, side) for side in range(2)]

    def start(*stages):
        for lag, copies in stages:
            on, at, slot = stage(lag)

            @pl.when(on)
            def _():
                for cp in copies(slot, at):
                    cp.start()

    start((PAIRED, sides_of(first_copy)), (FOLDED, sides_of(second_copy)), (FINAL, gather_1))

    @pl.when(step < tiles)
    def _():
        pair = lax.rem(step, 2)
        for s, ref in enumerate((dg_ref, du_ref)):
            for half_, to in ((0, out), (1, keep)):
                term = mm(at_ref[half_ * (d // 2) : (half_ + 1) * (d // 2), :], ref[...]).astype(bf16)
                for x in range(chips):
                    to[pair, x, s] = term[x * r : (x + 1) * r]
        down_ref[...] = lax.dot_general(act_ref[...], dy_ref[...], TNN, preferred_element_type=f32).astype(bf16)

    for lag, copies in ((DONE, gather_3), (ACROSS, gather_2), (SPREAD, gather_1)):
        on, at, slot = stage(lag)

        @pl.when(on)
        def _():
            for cp in copies(slot, at):
                cp.wait()

    start((SPREAD, gather_2), (ACROSS, gather_3))

    @pl.when(step < tiles)
    def _():
        pair_copy(lax.rem(step, 2)).start()


def grads(a, dy, w_gate, w_up, w_down, state, l, chips, wanted, name):
    t, d = a.shape
    f = w_down.shape[1]
    tiles = f // TN
    r = d // (2 * chips)
    whole = pl.BlockSpec((t, d), lambda j: (0, 0))

    def at(j):
        return jnp.minimum(j, tiles - 1)

    tile = pl.BlockSpec((t, TN), lambda j: (0, at(j)))
    wspec = pl.BlockSpec((None, d, TN), lambda j: (l, 0, at(j)))
    dspec = pl.BlockSpec((None, TN, d), lambda j: (l, at(j), 0))

    def late(j):
        return jnp.clip(j - FINAL, 0, tiles - 1)

    sspec = pl.BlockSpec((None, r, TN), lambda j: (l, 0, late(j)))
    out_specs = [pl.BlockSpec((TN, d), lambda j: (at(j), 0)), pl.BlockSpec((2, r, TN), lambda j: (0, 0, late(j)))]
    out_specs.append(pl.BlockSpec(memory_space=pl.ANY))
    out_shape = [sds((f, d), bf16), sds((2, r, f), bf16), sds((2, chips, 2, r, f), bf16)]
    scratch = [pltpu.VMEM((t, TN), bf16)] * 2
    if wanted:
        out_specs, out_shape, scratch = [tile, tile] + out_specs, [sds((t, f), bf16)] * 2 + out_shape, []
    dma = pltpu.SemaphoreType.DMA
    scratch += [
        pltpu.VMEM((d, t), bf16),
        pltpu.VMEM((t, TN), bf16),
        pltpu.VMEM((2, chips, 2, r, TN), bf16),
        pltpu.VMEM((2, chips, 2, r, TN), bf16),
        pltpu.VMEM((2, chips, 2, r, TN), bf16),
        pltpu.VMEM((SLOTS, 2, 2, r // 2, TN), bf16),
        pltpu.VMEM((SLOTS, 2, 2, r, TN), bf16),
        pltpu.VMEM((SLOTS, 2, r, TN), bf16),
        pltpu.VMEM((SLOTS, 2, 2, r, TN), bf16),
        pltpu.VMEM((SLOTS, 2, 2, r // 2, TN), bf16),
        pltpu.VMEM((SLOTS, 2, r, TN), bf16),
        dma((2, 2)),
        dma((2, 2, SLOTS)),
        dma((2, 2, SLOTS)),
        dma((8, 2, SLOTS)),
        dma((SLOTS,)),
    ]
    return pl.pallas_call(
        functools.partial(grads_kernel, chips, tiles, wanted),
        name=f"grads_{name}",
        grid=(tiles + DONE,),
        in_specs=[whole, whole, wspec, wspec, dspec] + [sspec] * 6,
        out_specs=out_specs,
        out_shape=out_shape,
        scratch_shapes=scratch,
        compiler_params=params(collective_id=l, has_side_effects=True),
        cost_estimate=cost(12 * t * d * f, 20 * t * f),
    )(a, dy, w_gate, w_up, w_down, *state)


def dh_kernel(cuts, *refs):
    n = len(cuts)
    dgs, dus, (wg_ref, wu_ref, h_ref, dy_ref, out_ref) = refs[:n], refs[n : 2 * n], refs[2 * n :]
    da = None
    for dg, du, (lo, hi) in zip(dgs, dus, cuts):
        for g, w in ((dg, wg_ref), (du, wu_ref)):
            term = lax.dot_general(g[...], w[:, lo:hi], NT, preferred_element_type=f32)
            da = term if da is None else da + term
    da = da.astype(bf16).astype(f32)
    wide = h_ref[...].astype(f32)
    scale = lax.rsqrt(jnp.mean(wide * wide, -1, keepdims=True) + 1e-6)
    norm = wide * scale
    back_ = scale * (da - norm * jnp.mean(da * norm, -1, keepdims=True))
    out_ref[...] = (dy_ref[...].astype(f32) + back_.astype(bf16).astype(f32)).astype(bf16)


def dh(dgs, dus, w_gate, w_up, h, dy, l):
    t, d = h.shape
    f = w_gate.shape[2]
    tm = 256
    cuts, at = [], 0
    for g in dgs:
        cuts.append((at, at + g.shape[1]))
        at += g.shape[1]
    row = pl.BlockSpec((tm, d), lambda i: (i, 0))
    chunks = [pl.BlockSpec((tm, g.shape[1]), lambda i: (i, 0)) for g in dgs]
    wspec = pl.BlockSpec((None, d, f), lambda i: (l, 0, 0))
    return pl.pallas_call(
        functools.partial(dh_kernel, tuple(cuts)),
        name=f"grad_input_{l}",
        grid=(t // tm,),
        in_specs=chunks + chunks + [wspec, wspec, row, row],
        out_specs=row,
        out_shape=sds((t, d), bf16),
        compiler_params=params(),
        cost_estimate=cost(4 * t * d * f, 4 * d * f + 4 * t * f + 6 * t * d),
    )(*dgs, *dus, w_gate, w_up, h, dy)


def width(c):
    return c // 2 if c % 256 == 0 else c


def pair_kernel(chips, got_ref, keep_ref, across_a, across_b, right, left, own):
    me = lax.axis_index("dp")
    chip, core = me // 2, lax.rem(me, 2)
    half = got_ref.shape[1] // 2

    def total(hop):
        i = lax.rem(chip + hop, chips)
        mine = keep_ref[i, core] if len(keep_ref.shape) == 4 else keep_ref[i]
        return (mine.astype(f32) + got_ref[i].astype(f32)).astype(bf16)

    across = total(2)
    across_a[...] = across[:half]
    across_b[...] = across[half:]
    right[...] = total(1)
    left[...] = total(3)
    own[...] = total(0)


def pair_add(got, keep, name):
    s, chips, r, c = got.shape
    tc = width(c)
    whole = pl.BlockSpec((None, chips, r, tc), lambda i, j: (i, 0, 0, j))
    wide = pl.BlockSpec((None, chips, 2, r, tc), lambda i, j: (i, 0, 0, 0, j)) if keep.ndim == 5 else whole
    one = pl.BlockSpec((None, r, tc), lambda i, j: (i, 0, j))
    half = pl.BlockSpec((None, r // 2, tc), lambda i, j: (i, 0, j))
    return pl.pallas_call(
        functools.partial(pair_kernel, chips),
        name=f"pair_add_{name}",
        grid=(s, c // tc),
        in_specs=[whole, wide],
        out_specs=[half, half, one, one, one],
        out_shape=[sds((s, r // 2, c), bf16)] * 2 + [sds((s, r, c), bf16)] * 3,
        compiler_params=params(),
        cost_estimate=cost(16 * s * r * c, 24 * s * r * c),
    )(got, keep)


def fold_kernel(right, left, a, b, right_out, left_out):
    right_out[...] = (right[...].astype(f32) + a[...].astype(f32)).astype(bf16)
    left_out[...] = (left[...].astype(f32) + b[...].astype(f32)).astype(bf16)


def fold(right, left, a, b, name):
    s, r, c = right.shape
    tc = width(c)
    lo = pl.BlockSpec((None, r // 2, tc), lambda i, j: (i, 0, j))
    hi = pl.BlockSpec((None, r // 2, tc), lambda i, j: (i, 1, j))
    return pl.pallas_call(
        fold_kernel,
        name=f"fold_{name}",
        grid=(s, c // tc),
        in_specs=[lo, hi, lo, lo],
        out_specs=[lo, hi],
        out_shape=[sds((s, r, c), bf16)] * 2,
        input_output_aliases={0: 0, 1: 1},
        compiler_params=params(),
        cost_estimate=cost(4 * s * r * c, 6 * s * r * c),
    )(right, left, a, b)


def adamw_kernel(n, *refs):
    sums, (w_ref, m_ref, v_ref), (nw_ref, nm_ref, nv_ref) = refs[:n], refs[n : n + 3], refs[-3:]
    g = sums[0][...].astype(f32)
    for other in sums[1:]:
        g = g + other[...].astype(f32)
    g = g.astype(bf16).astype(f32)
    m = 0.9 * m_ref[...] + 0.1 * g
    v = 0.95 * v_ref[...] + 0.05 * g * g
    w = w_ref[...].astype(f32)
    nm_ref[...] = m
    nv_ref[...] = v
    nw_ref[...] = (w - 0.02 * (m * lax.rsqrt(v + 1e-8) + 0.1 * w)).astype(bf16)


def adamw(sums, s, w, m, v, l, col, moments, new, name):
    n, r, c = sums[0].shape
    tr, tc = r // 2, TN if col or c < m.shape[2] else width(c)
    part = pl.BlockSpec((None, tr, tc), lambda i, j: (s, i, j))
    block = pl.BlockSpec((None, tr, tc), lambda i, j: (l, i, j + col // tc))
    anyspec = pl.BlockSpec(memory_space=pl.ANY)
    more, alias = [], {}
    for at, t in ((0, new),) + ((1, None), (2, None)) if moments is None else ((0, new), (1, moments[0]), (2, moments[1])):
        if t is not None:
            alias[len(sums) + 3 + len(more)] = at
            more.append(t)
    return pl.pallas_call(
        functools.partial(adamw_kernel, len(sums)),
        name=f"adamw_{name}",
        grid=(r // tr, c // tc),
        in_specs=[part] * len(sums) + [block] * 3 + [anyspec] * len(more),
        out_specs=[part, block, block],
        out_shape=[sds((n, r, c), bf16), sds(m.shape, f32), sds(v.shape, f32)],
        input_output_aliases=alias,
        compiler_params=params(),
        cost_estimate=cost(20 * r * c, 30 * r * c),
    )(*sums, w, m, v, *more)


def moments_kernel(g_ref, m_ref, v_ref, *rest):
    nm_ref, nv_ref = rest[-2:]
    g = g_ref[...].astype(f32)
    nm_ref[...] = 0.9 * m_ref[...] + 0.1 * g
    nv_ref[...] = 0.95 * v_ref[...] + 0.05 * g * g


def new_moments(g, s, m, v, l, into, name):
    _, r, c = g.shape
    tr, tc = r // 2, width(c)
    part = pl.BlockSpec((None, tr, tc), lambda i, j: (s, i, j))
    block = pl.BlockSpec((None, tr, tc), lambda i, j: (l, i, j))
    more = [] if into is None else list(into)
    return pl.pallas_call(
        moments_kernel,
        name=f"moments_{name}",
        grid=(r // tr, c // tc),
        in_specs=[part, block, block] + [pl.BlockSpec(memory_space=pl.ANY)] * len(more),
        out_specs=[block, block],
        out_shape=[sds(m.shape, f32), sds(v.shape, f32)],
        input_output_aliases={3: 0, 4: 1} if more else {},
        compiler_params=params(),
        cost_estimate=cost(10 * r * c, 18 * r * c),
    )(g, m, v, *more)


def stack_kernel(full_ref, *rest):
    for s, out in enumerate(rest[-2:]):
        out[...] = full_ref[s]


def stack_layer(full, layers, l, into, name):
    _, d, f = full.shape
    tr = d // 8
    more = [t for t in into if t is not None]
    block = pl.BlockSpec((None, tr, f), lambda i: (l, i, 0))
    return pl.pallas_call(
        stack_kernel,
        name=f"stack_{name}",
        grid=(d // tr,),
        in_specs=[pl.BlockSpec((2, tr, f), lambda i: (0, i, 0))] + [pl.BlockSpec(memory_space=pl.ANY)] * len(more),
        out_specs=[block, block],
        out_shape=[sds((layers, d, f), bf16)] * 2,
        input_output_aliases={1 + i: i for i in range(len(more))},
        compiler_params=params(),
        cost_estimate=cost(2 * d * f, 8 * d * f),
    )(full, *more)


def place_kernel(l, col, chips, kinds, n, k, *refs):
    pieces = refs[:n]
    refs = refs[n:]
    bufs, (isem, osem) = refs[-n - 2 : -2], refs[-2:]
    outs = refs[-n - 2 - k : -n - 2]
    me = lax.axis_index("dp")
    x, core = me // 2, lax.rem(me, 2)
    ins = []
    for i in range(n):
        cp = pltpu.make_async_copy(pieces[i], bufs[i], isem.at[i])
        cp.start()
        ins.append(cp)
    going = []
    for i, (hop, other, lo, hi) in enumerate(kinds):
        ins[i].wait()
        xi = lax.rem(x + hop, chips)
        ci = 1 - core if other else core
        for s, out in enumerate(outs):
            dst = out.at[l, xi, ci, pl.ds(lo, hi - lo), pl.ds(col, pieces[i].shape[2])]
            cp = pltpu.make_async_copy(bufs[i].at[s], dst, osem.at[i, s])
            cp.start()
            going.append(cp)
    for cp in going:
        cp.wait()


def place(pieces, kinds, shapes, l, col, into, chips, name):
    n, k = len(pieces), len(shapes)
    into = [t for t in into if t is not None]
    anyspec = pl.BlockSpec(memory_space=pl.ANY)
    moved = sum(p.size for p in pieces)
    return pl.pallas_call(
        functools.partial(place_kernel, l, col, chips, tuple(kinds), n, k),
        name=f"place_{name}",
        in_specs=[anyspec] * (n + len(into)),
        out_specs=[anyspec] * k,
        out_shape=[sds(shape, bf16) for shape in shapes],
        scratch_shapes=[pltpu.VMEM(p.shape, bf16) for p in pieces] + [pltpu.SemaphoreType.DMA((n,)), pltpu.SemaphoreType.DMA((n, k))],
        input_output_aliases={n + i: i for i in range(len(into))},
        compiler_params=params(),
        cost_estimate=cost(moved, 4 * moved),
    )(*pieces, *into)


def solution(mesh):
    n = mesh.shape["dp"]
    chips = n // 2
    PAIR = [(i, i ^ 1) for i in range(n)]
    RIGHT = [(i, (i + 2) % n) for i in range(n)]
    LEFT = [(i, (i - 2) % n) for i in range(n)]

    def send(t, way):
        return lax.ppermute(t, "dp", way)

    def body(x, dy, w_gate, w_up, w_down, m_gate, m_up, m_down, v_gate, v_up, v_down):
        me = lax.axis_index("dp")
        core = me % 2
        x, dy = x[0], dy[0]
        layers, d, f = w_gate.shape
        tiles = f // TN

        def block_of(w):
            r = w.shape[1] // n
            return lax.dynamic_slice_in_dim(w, me * r, r, 1)

        own_w = {"gate": block_of(w_gate), "up": block_of(w_up), "down": block_of(w_down)}
        m_in = {"gate": m_gate, "up": m_up, "down": m_down}
        v_in = {"gate": v_gate, "up": v_up, "down": v_down}
        moments, new_w = {}, {}

        class Unit:
            def __init__(self, keys, l, col, name, out=None, keep=None, total=None):
                self.keep, self.keys, self.l, self.col, self.name = keep, keys, l, col, name
                self.stage = 0
                if total is None:
                    self.flight = [send(out, PAIR)]
                else:
                    self.own, self.flight, self.stage = total, [], 2
                    self.advance()

            def advance(self):
                getattr(self, ("reduce_1", "reduce_2", "step", "gather_2", "gather_3", "finish")[self.stage])()
                self.stage += 1

            def reduce_1(self):
                a, b, self.right, self.left, self.own = pair_add(self.flight[0], self.keep, self.name)
                self.flight = [send(a, RIGHT), send(b, LEFT)]

            def reduce_2(self):
                right, left = fold(self.right, self.left, *self.flight, self.name)
                self.flight = [send(right, RIGHT), send(left, LEFT)]

            def step(self):
                w = None
                sums = [self.own, *self.flight]
                for s, key in enumerate(self.keys):
                    w, *moments[key] = adamw(
                        sums, s, own_w[key], m_in[key], v_in[key], self.l, self.col, moments.get(key), w, f"{self.name}_{key}"
                    )
                self.w = w
                self.flight = [send(w, RIGHT), send(w, LEFT), send(w, PAIR)]

            def gather_2(self):
                wl, wr, pw = self.flight
                half = wl.shape[1] // 2
                self.pieces = [self.w, wl, wr, pw]
                self.flight = [send(wl[:, :half], RIGHT), send(wr[:, half:], LEFT), send(wl, PAIR), send(wr, PAIR)]

            def gather_3(self):
                o1, o2, pwl, pwr = self.flight
                self.pieces += [pwl, pwr, o1, o2]
                self.flight = [send(o1, PAIR), send(o2, PAIR)]

            def finish(self):
                pieces = self.pieces + self.flight
                r = self.w.shape[1]
                half = r // 2
                kinds = [(0, False, 0, r), (3, False, 0, r), (1, False, 0, r), (0, True, 0, r), (3, True, 0, r), (1, True, 0, r)]
                kinds += [(2, o, lo, hi) for o in (False, True) for lo, hi in ((0, half), (half, r))]
                shapes = [(layers, chips, 2, r, own_w[key].shape[2]) for key in self.keys]
                into = [new_w.get(key) for key in self.keys]
                for key, t in zip(self.keys, place(pieces, kinds, shapes, self.l, self.col, into, chips, self.name)):
                    new_w[key] = t

        def after(units, *inputs):
            inputs, flights = lax.optimization_barrier((inputs, [u.flight for u in units]))
            for u, flight in zip(units, flights):
                u.flight = flight
                u.advance()
            return inputs

        def down_unit(g, l):
            g = g.reshape(1, chips, 2, f // n, d)
            out = lax.dynamic_index_in_dim(g, 1 - core, 2, keepdims=False)
            return Unit(("down",), l, 0, f"{l}d", out, g)

        kept = []
        h = x
        for l in range(layers - 1):
            a, act = fwd(h, w_gate, w_up, l)
            kept.append((h, a))
            h, a = down(h, act, w_down, l)
        l = layers - 1
        def state_of():
            return [t[k] for k in ("gate", "up") for t in (own_w, m_in, v_in)]

        def moments_of(g, l):
            for i, key in enumerate(("gate", "up")):
                moments[key] = new_moments(g, i, m_in[key], v_in[key], l, moments.get(key), f"{l}_{key}")

        def stack_of(full, l):
            full = full.reshape(2, d, f)
            new_w["gate"], new_w["up"] = stack_layer(full, layers, l, (new_w.get("gate"), new_w.get("up")), f"{l}")

        def beside(unit, *work):
            for f_, *args in work:
                f_(*args)
            unit.flight, moments_, new_w_ = lax.optimization_barrier((unit.flight, dict(moments), dict(new_w)))
            moments.update(moments_)
            new_w.update(new_w_)
            unit.advance()

        dg, du, g_down, total, full_w = grads(a, dy, w_gate, w_up, w_down, state_of(), l, chips, True, f"{l}")
        done = []
        for l in range(layers - 2, -1, -1):
            unit = down_unit(g_down, l + 1)
            dg, du = after([unit], dg, du)
            dy = dh([dg], [du], w_gate, w_up, h, dy, l + 1)
            h, a = kept[l]
            (dy,) = after([unit], dy)
            done.append((total, full_w, l + 1))
            dg = du = None
            g_down, total, full_w = grads(a, dy, w_gate, w_up, w_down, state_of(), l, chips, False, f"{l}")
            (g_down,) = after([unit], g_down)
            g_down, unit.w = lax.optimization_barrier((g_down, unit.w))
        done.append((total, full_w, 0))
        tail = down_unit(g_down, 0)
        (g1, f1, l1), (g0, f0, l0) = done
        beside(tail)
        beside(tail, (moments_of, g1, l1))
        beside(unit)
        beside(tail, (stack_of, f1, l1), (moments_of, g0, l0))
        beside(unit)
        beside(unit)
        beside(tail, (stack_of, f0, l0))
        while tail.stage < 6:
            tail.advance()
        keys = ("gate", "up", "down")
        ws = tuple(new_w[k].reshape(w.shape) for k, w in zip(keys, (w_gate, w_up, w_down)))
        return ws + tuple(moments[k][0] for k in keys) + tuple(moments[k][1] for k in keys)

    seq, full, rows = P(("rep", "dp")), P(), P(None, "dp")
    out_m = P("rep", "dp")
    return jax.shard_map(
        body,
        mesh=mesh,
        in_specs=(seq, seq) + (full,) * 3 + (rows,) * 6,
        out_specs=(P("rep"),) * 3 + (out_m,) * 6,
        check_vma=False,
    )
```

```python
import functools

import jax
import jax.numpy as jnp
from jax import lax
from jax.experimental import pallas as pl
from jax.experimental.pallas import tpu as pltpu
from jax.sharding import PartitionSpec as P

f32 = jnp.float32
bf16 = jnp.bfloat16
VMEM_LIMIT = 60 * 1024 * 1024
TN = 256


def params(**kw):
    return pltpu.CompilerParams(vmem_limit_bytes=VMEM_LIMIT, **kw)


def cost(flops, bytes_accessed):
    return pl.CostEstimate(flops=flops, bytes_accessed=bytes_accessed, transcendentals=0)


def sds(shape, dtype):
    return jax.ShapeDtypeStruct(shape, dtype)


NT = (((1,), (1,)), ((), ()))
TNN = (((0,), (0,)), ((), ()))


def mm(a, b):
    return jnp.dot(a, b, preferred_element_type=f32)


def fwd_kernel(rows, x_ref, wg_ref, wu_ref, a_ref, act_ref):
    t = x_ref.shape[0]

    @pl.when(pl.program_id(0) == 0)
    def _():
        for r in range(0, t, rows):
            wide = x_ref[r : r + rows, :].astype(f32)
            scale = lax.rsqrt(jnp.mean(wide * wide, -1, keepdims=True) + 1e-6)
            a_ref[r : r + rows, :] = (wide * scale).astype(bf16)

    for r in range(0, t, rows):
        a = a_ref[r : r + rows, :]
        g = mm(a, wg_ref[...])
        u = mm(a, wu_ref[...])
        act_ref[r : r + rows, :] = (g * jax.nn.sigmoid(g) * u).astype(bf16)


def fwd(x, w_gate, w_up, l):
    t, d = x.shape
    f = w_gate.shape[2]
    whole = pl.BlockSpec((t, d), lambda j: (0, 0))
    wspec = pl.BlockSpec((None, d, TN), lambda j: (l, 0, j))
    tile = pl.BlockSpec((t, TN), lambda j: (0, j))
    return pl.pallas_call(
        functools.partial(fwd_kernel, 512),
        name=f"fwd_gate_up_{l}",
        grid=(f // TN,),
        in_specs=[whole, wspec, wspec],
        out_specs=[whole, tile],
        out_shape=[sds((t, d), bf16), sds((t, f), bf16)],
        compiler_params=params(),
        cost_estimate=cost(4 * t * d * f, 4 * d * f + 2 * t * f + 4 * t * d),
    )(x, w_gate, w_up)


def down_kernel(x_ref, act_ref, w_ref, h_ref, a_ref):
    y = mm(act_ref[...], w_ref[...]).astype(bf16)
    h = (x_ref[...].astype(f32) + y.astype(f32)).astype(bf16)
    h_ref[...] = h
    wide = h.astype(f32)
    scale = lax.rsqrt(jnp.mean(wide * wide, -1, keepdims=True) + 1e-6)
    a_ref[...] = (wide * scale).astype(bf16)


def down(x, act, w_down, l):
    t, d = x.shape
    f = act.shape[1]
    tm = 256
    row = pl.BlockSpec((tm, d), lambda i: (i, 0))
    return pl.pallas_call(
        down_kernel,
        name=f"down_{l}",
        grid=(t // tm,),
        in_specs=[row, pl.BlockSpec((tm, f), lambda i: (i, 0)), pl.BlockSpec((None, f, d), lambda i: (l, 0, 0))],
        out_specs=[row, row],
        out_shape=[sds((t, d), bf16), sds((t, d), bf16)],
        compiler_params=params(),
        cost_estimate=cost(2 * t * d * f, 2 * d * f + 2 * t * f + 6 * t * d),
    )(x, act, w_down)


def silu_back(g, u, dact):
    s = jax.nn.sigmoid(g)
    gs = g * s
    dgate = dact * u * (s + gs * (1.0 - s))
    return dgate.astype(bf16), (dact * gs).astype(bf16)


PAIRED, FOLDED, FINAL, SPREAD, ACROSS, DONE = 1, 2, 3, 4, 5, 6
SLOTS = 4


class Stream:
    def __init__(self, chips, tiles, refs, full, g_ref, state, at_place):
        self.out, self.keep, self.got, self.across, self.near, self.own = refs[:6]
        self.from_near, self.from_far, self.fresh, self.psem, self.sem1, self.sem2, self.gsem, self.lsem = refs[6:]
        self.chips, self.tiles, self.full, self.g_ref, self.state, self.at_place = chips, tiles, full, g_ref, state, at_place
        self.r = self.own.shape[2]
        self.half = self.r // 2
        me = lax.axis_index("dp")
        n = 2 * chips
        self.chip, self.core = me // 2, lax.rem(me, 2)
        self.partner = self.chip * 2 + 1 - self.core
        self.sides = (lax.rem(me + 2, n), lax.rem(me + n - 2, n))
        self.step = pl.program_id(0)

    @staticmethod
    def scratch(chips, s, r, c):
        dma = pltpu.SemaphoreType.DMA
        return [
            pltpu.VMEM((2, chips, s, r, c), bf16),
            pltpu.VMEM((2, chips, s, r, c), bf16),
            pltpu.VMEM((2, chips, s, r, c), bf16),
            pltpu.VMEM((SLOTS, 2, s, r // 2, c), bf16),
            pltpu.VMEM((SLOTS, 2, s, r, c), bf16),
            pltpu.VMEM((SLOTS, s, r, c), bf16),
            pltpu.VMEM((SLOTS, 2, s, r, c), bf16),
            pltpu.VMEM((SLOTS, 2, s, r // 2, c), bf16),
            pltpu.VMEM((SLOTS, s, r, c), bf16),
            dma((2, 2)),
            dma((2, 2, SLOTS)),
            dma((2, 2, SLOTS)),
            dma((8, 2, SLOTS)),
            dma((SLOTS,)),
        ]

    def greet(self):
        barrier = pltpu.get_barrier_semaphore()
        for to in (self.partner, *self.sides):
            pl.semaphore_signal(barrier, inc=1, device_id={"dp": to}, device_id_type=pl.DeviceIdType.MESH)
        pl.semaphore_wait(barrier, 3)

    def remote(self, src, dst, sems, slot, to):
        return pltpu.make_async_remote_copy(
            src_ref=src,
            dst_ref=dst,
            send_sem=sems.at[0, slot],
            recv_sem=sems.at[1, slot],
            device_id={"dp": to},
            device_id_type=pl.DeviceIdType.MESH,
        )

    def pair_copy(self, pair):
        return self.remote(self.out.at[pair], self.got.at[pair], self.psem, pair, self.partner)

    def first(self, slot, at):
        return [
            self.remote(self.across.at[slot, i], self.from_far.at[slot, i], self.sem1.at[i], slot, to) for i, to in enumerate(self.sides)
        ]

    def second(self, slot, at):
        return [self.remote(self.near.at[slot, i], self.from_near.at[slot, i], self.sem2.at[i], slot, to) for i, to in enumerate(self.sides)]

    def place(self, hop, at, lo=0, hi=None):
        return self.at_place(self.full, lax.rem(self.chip + hop, self.chips), self.core, at, lo, self.r if hi is None else hi)

    def gather_1(self, slot, at):
        here, new = self.place(0, at), self.fresh.at[slot]
        ways = [self.remote(new, here, self.gsem.at[i], slot, to) for i, to in enumerate((*self.sides, self.partner))]
        return [*ways, pltpu.make_async_copy(new, here, self.lsem.at[slot])]

    def gather_2(self, slot, at):
        last, half = self.chips - 1, self.half
        before, ahead = self.place(last, at), self.place(1, at)
        low, high = self.place(last, at, 0, half), self.place(1, at, half, self.r)
        ways = ((low, self.sides[0]), (high, self.sides[1]), (before, self.partner), (ahead, self.partner))
        return [self.remote(ref, ref, self.gsem.at[3 + i], slot, to) for i, (ref, to) in enumerate(ways)]

    def gather_3(self, slot, at):
        far = self.place(self.chips // 2, at)
        return [self.remote(far, far, self.gsem.at[7], slot, self.partner)]

    def stage(self, lag):
        at = self.step - lag
        return (at >= 0) & (at < self.tiles), at, lax.rem(jnp.maximum(at, 0), SLOTS)

    def each(self, what, *stages):
        for lag, copies in stages:
            on, at, slot = self.stage(lag)

            @pl.when(on)
            def _():
                for cp in copies(slot, at):
                    getattr(cp, what)()

    def reduce(self):
        half = self.half

        def add(x, y):
            return (x.astype(f32) + y.astype(f32)).astype(bf16)

        on, at, slot = self.stage(FINAL)

        @pl.when(on)
        def _():
            for cp in self.second(slot, at):
                cp.wait()
            total = self.own[slot].astype(f32) + self.from_near[slot, 0].astype(f32) + self.from_near[slot, 1].astype(f32)
            total = total.astype(bf16)
            self.g_ref[...] = total
            for i, (w_ref, m_ref, v_ref) in enumerate(self.state):
                g = total[i].astype(f32)
                m = 0.9 * m_ref[...] + 0.1 * g
                v = 0.95 * v_ref[...] + 0.05 * g * g
                w = w_ref[...].astype(f32)
                self.fresh[slot, i] = (w - 0.02 * (m * lax.rsqrt(v + 1e-8) + 0.1 * w)).astype(bf16)

        on, at, slot = self.stage(FOLDED)

        @pl.when(on)
        def _():
            for cp in self.first(slot, at):
                cp.wait()
            self.near[slot, 0, :, :half] = add(self.near[slot, 0, :, :half], self.from_far[slot, 0])
            self.near[slot, 1, :, half:] = add(self.near[slot, 1, :, half:], self.from_far[slot, 1])

        on, at, slot = self.stage(PAIRED)

        @pl.when(on)
        def _():
            pair = lax.rem(at, 2)
            self.pair_copy(pair).wait()

            def total(hop):
                i = lax.rem(self.chip + hop, self.chips)
                return add(self.keep[pair, i], self.got[pair, i])

            far = total(self.chips // 2)
            self.across[slot, 0] = far[:, :half]
            self.across[slot, 1] = far[:, half:]
            self.near[slot, 0] = total(1)
            self.near[slot, 1] = total(self.chips - 1)
            self.own[slot] = total(0)

        self.each("start", (PAIRED, self.first), (FOLDED, self.second), (FINAL, self.gather_1))

    def gather(self):
        self.each("wait", (DONE, self.gather_3), (ACROSS, self.gather_2), (SPREAD, self.gather_1))
        self.each("start", (SPREAD, self.gather_2), (ACROSS, self.gather_3))

        @pl.when(self.step < self.tiles)
        def _():
            self.pair_copy(lax.rem(self.step, 2)).start()


def grads_kernel(chips, tiles, wanted, *refs):
    a_ref, dy_ref, p_ref, q_ref, wd_ref = refs[:5]
    state = (refs[5:8], refs[8:11])
    refs = refs[11:]
    if wanted:
        (h_ref, dh_ref), refs = (refs[0], refs[1]), refs[2:]
        da_ref, refs = refs[3], refs[:3] + refs[4:]
    down_ref, g_ref, full, dg_ref, du_ref, at_ref, act_ref = refs[:7]
    t, d = a_ref.shape
    r = d // (2 * chips)

    def at_place(full, x, core, at, lo, hi):
        return full.at[:, x, core, pl.ds(lo, hi - lo), pl.ds(pl.multiple_of(at * TN, TN), TN)]

    group = Stream(chips, tiles, refs[7:], full, g_ref, state, at_place)
    step, core = group.step, group.core

    @pl.when(step == 0)
    def _():
        group.greet()
        if wanted:
            da_ref[...] = jnp.zeros_like(da_ref)
        for part, which in enumerate((1 - core, core)):
            for x in range(chips):
                at = pl.multiple_of((2 * x + which) * r, 128)
                to = (part * chips + x) * r
                at_ref[to : to + r, :] = a_ref[:, pl.ds(at, r)].T

    @pl.when(step < tiles)
    def _():
        rows = 512
        for lo in range(0, t, rows):
            at = slice(lo, lo + rows)
            g, u = mm(a_ref[at, :], p_ref[...]), mm(a_ref[at, :], q_ref[...])
            dact = lax.dot_general(dy_ref[at, :], wd_ref[...], NT, preferred_element_type=f32)
            act_ref[at, :] = (g * jax.nn.sigmoid(g) * u).astype(bf16)
            dg_ref[at, :], du_ref[at, :] = silu_back(g, u, dact.astype(bf16).astype(f32))

    group.reduce()

    if wanted:
        rows = 512

        @pl.when(step < tiles)
        def _():
            for lo in range(0, t, rows):
                at = slice(lo, lo + rows)
                term = lax.dot_general(dg_ref[at, :], p_ref[...], NT, preferred_element_type=f32)
                da_ref[at, :] += term + lax.dot_general(du_ref[at, :], q_ref[...], NT, preferred_element_type=f32)

        @pl.when(step == tiles)
        def _():
            for lo in range(0, t, rows):
                at = slice(lo, lo + rows)
                da = da_ref[at, :].astype(bf16).astype(f32)
                wide = h_ref[at, :].astype(f32)
                scale = lax.rsqrt(jnp.mean(wide * wide, -1, keepdims=True) + 1e-6)
                norm = wide * scale
                back_ = scale * (da - norm * jnp.mean(da * norm, -1, keepdims=True))
                dh_ref[at, :] = (dy_ref[at, :].astype(f32) + back_.astype(bf16).astype(f32)).astype(bf16)

    @pl.when(step < tiles)
    def _():
        pair = lax.rem(step, 2)
        for s, ref in enumerate((dg_ref, du_ref)):
            for part, to in ((0, group.out), (1, group.keep)):
                term = mm(at_ref[part * (d // 2) : (part + 1) * (d // 2), :], ref[...]).astype(bf16)
                for x in range(chips):
                    to[pair, x, s] = term[x * r : (x + 1) * r]
        down_ref[...] = lax.dot_general(act_ref[...], dy_ref[...], TNN, preferred_element_type=f32).astype(bf16)

    group.gather()


def grads(a, dy, w_gate, w_up, w_down, state, h, l, chips, name):
    wanted = h is not None
    t, d = a.shape
    f = w_down.shape[1]
    tiles = f // TN
    r = d // (2 * chips)
    whole = pl.BlockSpec((t, d), lambda j: (0, 0), pipeline_mode=pl.Buffered(1))

    def at(j):
        return jnp.minimum(j, tiles - 1)

    wspec = pl.BlockSpec((None, d, TN), lambda j: (l, 0, at(j)))
    dspec = pl.BlockSpec((None, TN, d), lambda j: (l, at(j), 0))

    def late(j):
        return jnp.clip(j - FINAL, 0, tiles - 1)

    sspec = pl.BlockSpec((None, r, TN), lambda j: (l, 0, late(j)))
    mine = pl.BlockSpec((None, r, TN), lambda j: (l, lax.axis_index("dp"), late(j)))
    out_specs = [pl.BlockSpec((TN, d), lambda j: (at(j), 0)), pl.BlockSpec((2, r, TN), lambda j: (0, 0, late(j)))]
    out_specs.append(pl.BlockSpec(memory_space=pl.ANY))
    out_shape = [sds((f, d), bf16), sds((2, r, f), bf16), sds((2, chips, 2, r, f), bf16)]
    scratch = [pltpu.VMEM((t, TN), bf16)] * 2
    more = []
    if wanted:
        out_specs, out_shape, more = [pl.BlockSpec((t, d), lambda j: (0, 0))] + out_specs, [sds((t, d), bf16)] + out_shape, [h]
        scratch = [pltpu.VMEM((t, d), f32)] + scratch
    scratch += [pltpu.VMEM((d, t), bf16), pltpu.VMEM((t, TN), bf16)] + Stream.scratch(chips, 2, r, TN)
    return pl.pallas_call(
        functools.partial(grads_kernel, chips, tiles, wanted),
        name=f"grads_{name}",
        grid=(tiles + DONE,),
        in_specs=[whole, whole, wspec, wspec, dspec] + [mine, sspec, sspec] * 2 + [whole] * len(more),
        out_specs=out_specs,
        out_shape=out_shape,
        scratch_shapes=scratch,
        compiler_params=params(collective_id=l, has_side_effects=True),
        cost_estimate=cost(12 * t * d * f, 20 * t * f),
    )(a, dy, w_gate, w_up, w_down, *state, *more)


def width(c):
    return c // 2 if c % 256 == 0 else c


def pair_kernel(chips, got_ref, keep_ref, across_a, across_b, right, left, own):
    me = lax.axis_index("dp")
    chip, core = me // 2, lax.rem(me, 2)
    half = got_ref.shape[1] // 2

    def total(hop):
        i = lax.rem(chip + hop, chips)
        mine = keep_ref[i, core] if len(keep_ref.shape) == 4 else keep_ref[i]
        return (mine.astype(f32) + got_ref[i].astype(f32)).astype(bf16)

    across = total(2)
    across_a[...] = across[:half]
    across_b[...] = across[half:]
    right[...] = total(1)
    left[...] = total(3)
    own[...] = total(0)


def pair_add(got, keep, name):
    s, chips, r, c = got.shape
    tc = width(c)
    whole = pl.BlockSpec((None, chips, r, tc), lambda i, j: (i, 0, 0, j))
    wide = pl.BlockSpec((None, chips, 2, r, tc), lambda i, j: (i, 0, 0, 0, j)) if keep.ndim == 5 else whole
    one = pl.BlockSpec((None, r, tc), lambda i, j: (i, 0, j))
    half = pl.BlockSpec((None, r // 2, tc), lambda i, j: (i, 0, j))
    return pl.pallas_call(
        functools.partial(pair_kernel, chips),
        name=f"pair_add_{name}",
        grid=(s, c // tc),
        in_specs=[whole, wide],
        out_specs=[half, half, one, one, one],
        out_shape=[sds((s, r // 2, c), bf16)] * 2 + [sds((s, r, c), bf16)] * 3,
        compiler_params=params(),
        cost_estimate=cost(16 * s * r * c, 24 * s * r * c),
    )(got, keep)


def fold_kernel(right, left, a, b, right_out, left_out):
    right_out[...] = (right[...].astype(f32) + a[...].astype(f32)).astype(bf16)
    left_out[...] = (left[...].astype(f32) + b[...].astype(f32)).astype(bf16)


def fold(right, left, a, b, name):
    s, r, c = right.shape
    tc = width(c)
    lo = pl.BlockSpec((None, r // 2, tc), lambda i, j: (i, 0, j))
    hi = pl.BlockSpec((None, r // 2, tc), lambda i, j: (i, 1, j))
    return pl.pallas_call(
        fold_kernel,
        name=f"fold_{name}",
        grid=(s, c // tc),
        in_specs=[lo, hi, lo, lo],
        out_specs=[lo, hi],
        out_shape=[sds((s, r, c), bf16)] * 2,
        input_output_aliases={0: 0, 1: 1},
        compiler_params=params(),
        cost_estimate=cost(4 * s * r * c, 6 * s * r * c),
    )(right, left, a, b)


def adamw_kernel(n, *refs):
    sums, (w_ref, m_ref, v_ref), (nw_ref, nm_ref, nv_ref) = refs[:n], refs[n : n + 3], refs[-3:]
    g = sums[0][...].astype(f32)
    for other in sums[1:]:
        g = g + other[...].astype(f32)
    g = g.astype(bf16).astype(f32)
    m = 0.9 * m_ref[...] + 0.1 * g
    v = 0.95 * v_ref[...] + 0.05 * g * g
    w = w_ref[...].astype(f32)
    nm_ref[...] = m
    nv_ref[...] = v
    nw_ref[...] = (w - 0.02 * (m * lax.rsqrt(v + 1e-8) + 0.1 * w)).astype(bf16)


def adamw(sums, s, w, m, v, l, col, moments, new, name):
    n, r, c = sums[0].shape
    tr, tc = r // 2, TN if col or c < m.shape[2] else width(c)
    part = pl.BlockSpec((None, tr, tc), lambda i, j: (s, i, j))
    block = pl.BlockSpec((None, tr, tc), lambda i, j: (l, i, j + col // tc))
    mine = pl.BlockSpec((None, tr, tc), lambda i, j: (l, lax.axis_index("dp") * (r // tr) + i, j + col // tc))
    anyspec = pl.BlockSpec(memory_space=pl.ANY)
    more, alias = [], {}
    for at, t in ((0, new),) + ((1, None), (2, None)) if moments is None else ((0, new), (1, moments[0]), (2, moments[1])):
        if t is not None:
            alias[len(sums) + 3 + len(more)] = at
            more.append(t)
    return pl.pallas_call(
        functools.partial(adamw_kernel, len(sums)),
        name=f"adamw_{name}",
        grid=(r // tr, c // tc),
        in_specs=[part] * len(sums) + [mine, block, block] + [anyspec] * len(more),
        out_specs=[part, block, block],
        out_shape=[sds((n, r, c), bf16), sds(m.shape, f32), sds(v.shape, f32)],
        input_output_aliases=alias,
        compiler_params=params(),
        cost_estimate=cost(20 * r * c, 30 * r * c),
    )(*sums, w, m, v, *more)


def moments_kernel(g_ref, m_ref, v_ref, *rest):
    nm_ref, nv_ref = rest[-2:]
    g = g_ref[...].astype(f32)
    nm_ref[...] = 0.9 * m_ref[...] + 0.1 * g
    nv_ref[...] = 0.95 * v_ref[...] + 0.05 * g * g


def new_moments(g, s, m, v, l, into, name):
    _, r, c = g.shape
    tr, tc = r // 2, width(c)
    part = pl.BlockSpec((None, tr, tc), lambda i, j: (s, i, j))
    block = pl.BlockSpec((None, tr, tc), lambda i, j: (l, i, j))
    more = [] if into is None else list(into)
    return pl.pallas_call(
        moments_kernel,
        name=f"moments_{name}",
        grid=(r // tr, c // tc),
        in_specs=[part, block, block] + [pl.BlockSpec(memory_space=pl.ANY)] * len(more),
        out_specs=[block, block],
        out_shape=[sds(m.shape, f32), sds(v.shape, f32)],
        input_output_aliases={3: 0, 4: 1} if more else {},
        compiler_params=params(),
        cost_estimate=cost(10 * r * c, 18 * r * c),
    )(g, m, v, *more)


def stack_kernel(k, full_ref, *rest):
    for s, out in enumerate(rest[-k:]):
        out[...] = full_ref[s]


def stack_layer(full, layers, l, into, name):
    k, d, f = full.shape
    tr = d // 8
    more = [t for t in into if t is not None]
    block = pl.BlockSpec((None, tr, f), lambda i: (l, i, 0))
    return pl.pallas_call(
        functools.partial(stack_kernel, k),
        name=f"stack_{name}",
        grid=(d // tr,),
        in_specs=[pl.BlockSpec((k, tr, f), lambda i: (0, i, 0))] + [pl.BlockSpec(memory_space=pl.ANY)] * len(more),
        out_specs=[block] * k,
        out_shape=[sds((layers, d, f), bf16)] * k,
        input_output_aliases={1 + i: i for i in range(len(more))},
        compiler_params=params(),
        cost_estimate=cost(k * d * f, 4 * k * d * f),
    )(full, *more)


def place_kernel(l, col, chips, kinds, n, k, *refs):
    pieces = refs[:n]
    refs = refs[n:]
    bufs, (isem, osem) = refs[-n - 2 : -2], refs[-2:]
    outs = refs[-n - 2 - k : -n - 2]
    me = lax.axis_index("dp")
    x, core = me // 2, lax.rem(me, 2)
    ins = []
    for i in range(n):
        cp = pltpu.make_async_copy(pieces[i], bufs[i], isem.at[i])
        cp.start()
        ins.append(cp)
    going = []
    for i, (hop, other, lo, hi) in enumerate(kinds):
        ins[i].wait()
        xi = lax.rem(x + hop, chips)
        ci = 1 - core if other else core
        for s, out in enumerate(outs):
            dst = out.at[l, xi, ci, pl.ds(lo, hi - lo), pl.ds(col, pieces[i].shape[2])]
            cp = pltpu.make_async_copy(bufs[i].at[s], dst, osem.at[i, s])
            cp.start()
            going.append(cp)
    for cp in going:
        cp.wait()


def place(pieces, kinds, shapes, l, col, into, chips, name):
    n, k = len(pieces), len(shapes)
    into = [t for t in into if t is not None]
    anyspec = pl.BlockSpec(memory_space=pl.ANY)
    moved = sum(p.size for p in pieces)
    return pl.pallas_call(
        functools.partial(place_kernel, l, col, chips, tuple(kinds), n, k),
        name=f"place_{name}",
        in_specs=[anyspec] * (n + len(into)),
        out_specs=[anyspec] * k,
        out_shape=[sds(shape, bf16) for shape in shapes],
        scratch_shapes=[pltpu.VMEM(p.shape, bf16) for p in pieces] + [pltpu.SemaphoreType.DMA((n,)), pltpu.SemaphoreType.DMA((n, k))],
        input_output_aliases={n + i: i for i in range(len(into))},
        compiler_params=params(),
        cost_estimate=cost(moved, 4 * moved),
    )(*pieces, *into)


def solution(mesh):
    n = mesh.shape["dp"]
    chips = n // 2
    PAIR = [(i, i ^ 1) for i in range(n)]
    RIGHT = [(i, (i + 2) % n) for i in range(n)]
    LEFT = [(i, (i - 2) % n) for i in range(n)]

    def send(t, way):
        return lax.ppermute(t, "dp", way)

    def body(x, dy, w_gate, w_up, w_down, m_gate, m_up, m_down, v_gate, v_up, v_down):
        me = lax.axis_index("dp")
        core = me % 2
        x, dy = x[0], dy[0]
        layers, d, f = w_gate.shape
        tiles = f // TN

        own_w = {"gate": w_gate, "up": w_up, "down": w_down}
        m_in = {"gate": m_gate, "up": m_up, "down": m_down}
        v_in = {"gate": v_gate, "up": v_up, "down": v_down}
        moments, new_w = {}, {}

        class Unit:
            def __init__(self, keys, l, col, name, out=None, keep=None, total=None):
                self.keep, self.keys, self.l, self.col, self.name = keep, keys, l, col, name
                self.stage, self.hold = 0, None
                if total is None:
                    self.flight = [send(out, PAIR)]
                else:
                    self.own, self.flight, self.stage = total, [], 2
                    self.advance()

            def advance(self):
                getattr(self, ("reduce_1", "reduce_2", "step", "gather_2", "gather_3", "finish")[self.stage])()
                self.stage += 1

            def reduce_1(self):
                a, b, self.right, self.left, self.own = pair_add(self.flight[0], self.keep, self.name)
                if self.hold is not None:
                    a, b, self.hold = lax.optimization_barrier((a, b, self.hold))
                self.flight = [send(a, RIGHT), send(b, LEFT)]

            def reduce_2(self):
                right, left = fold(self.right, self.left, *self.flight, self.name)
                if self.hold is not None:
                    right, left, self.hold = lax.optimization_barrier((right, left, self.hold))
                self.flight = [send(right, RIGHT), send(left, LEFT)]

            def step(self):
                w = None
                sums = [self.own, *self.flight]
                for s, key in enumerate(self.keys):
                    w, *moments[key] = adamw(
                        sums, s, own_w[key], m_in[key], v_in[key], self.l, self.col, moments.get(key), w, f"{self.name}_{key}"
                    )
                self.w = w
                self.flight = [send(w, RIGHT), send(w, LEFT), send(w, PAIR)]

            def gather_2(self):
                wl, wr, pw = self.flight
                half = wl.shape[1] // 2
                self.pieces = [self.w, wl, wr, pw]
                self.flight = [send(wl[:, :half], RIGHT), send(wr[:, half:], LEFT), send(wl, PAIR), send(wr, PAIR)]

            def gather_3(self):
                o1, o2, pwl, pwr = self.flight
                self.pieces += [pwl, pwr, o1, o2]
                self.flight = [send(o1, PAIR), send(o2, PAIR)]

            def finish(self):
                pieces = self.pieces + self.flight
                r = self.w.shape[1]
                half = r // 2
                kinds = [(0, False, 0, r), (3, False, 0, r), (1, False, 0, r), (0, True, 0, r), (3, True, 0, r), (1, True, 0, r)]
                kinds += [(2, o, lo, hi) for o in (False, True) for lo, hi in ((0, half), (half, r))]
                shapes = [(layers, chips, 2, r, own_w[key].shape[2]) for key in self.keys]
                into = [None if key not in new_w else new_w[key].reshape(shape) for key, shape in zip(self.keys, shapes)]
                for key, t in zip(self.keys, place(pieces, kinds, shapes, self.l, self.col, into, chips, self.name)):
                    new_w[key] = t

        def after(units, *inputs):
            inputs, flights = lax.optimization_barrier((inputs, [u.flight for u in units]))
            for u, flight in zip(units, flights):
                u.flight = flight
                u.advance()
            return inputs

        def down_unit(g, l):
            g = g.reshape(1, chips, 2, f // n, d)
            out = lax.dynamic_index_in_dim(g, 1 - core, 2, keepdims=False)
            return Unit(("down",), l, 0, f"{l}d", out, g)

        kept = []
        h = x
        for l in range(layers - 1):
            a, act = fwd(h, w_gate, w_up, l)
            kept.append((h, a))
            h, a = down(h, act, w_down, l)
        l = layers - 1
        def state_of(*keys):
            return [t[k] for k in keys for t in (own_w, m_in, v_in)]

        def moments_of(g, keys, l):
            for i, key in enumerate(keys):
                moments[key] = new_moments(g, i, m_in[key], v_in[key], l, moments.get(key), f"{l}_{key}")

        def stack_of(full, keys, l):
            full = full.reshape(len(keys), -1, full.shape[-1])
            for key, t in zip(keys, stack_layer(full, layers, l, [new_w.get(k) for k in keys], f"{l}_{keys[-1]}")):
                new_w[key] = t

        def beside(unit, *work):
            for f_, *args in work:
                f_(*args)
            made = [{k: v for k, v in vars(u).items() if k in ("own", "w")} for u in live]
            unit.flight, moments_, new_w_, made = lax.optimization_barrier((unit.flight, dict(moments), dict(new_w), made))
            moments.update(moments_)
            new_w.update(new_w_)
            for u, values in zip(live, made):
                vars(u).update(values)
            unit.advance()

        both = ("gate", "up")
        jobs, units, live = [], [], []
        for l in range(layers - 1, -1, -1):
            if units:
                units[-1].hold = dy
                beside(units[-1], jobs[-2])
                dy, units[-1].hold = units[-1].hold, None
            *cot, g_down, g, full = grads(a, dy, w_gate, w_up, w_down, state_of(*both), h if l else None, l, chips, f"{l}")
            jobs += [(moments_of, g, both, l), (stack_of, full, both, l)]
            if l:
                dy = cot[0]
                h, a = kept[l - 1]
                units.append(down_unit(g_down, l))
                live.append(units[-1])
        (unit,) = units
        unit.hold = g_down
        beside(unit)
        tail = down_unit(unit.hold, 0)
        unit.hold = None
        live.append(tail)
        beside(tail)
        beside(tail, jobs[2])
        beside(unit)
        beside(tail, jobs[1])
        beside(unit)
        beside(tail, jobs[3])
        beside(unit)
        unit.advance()
        while tail.stage < 6:
            tail.advance()
        keys = ("gate", "up", "down")
        ws = tuple(new_w[k].reshape(w.shape) for k, w in zip(keys, (w_gate, w_up, w_down)))
        return ws + tuple(moments[k][0] for k in keys) + tuple(moments[k][1] for k in keys)

    seq, full, rows = P(("rep", "dp")), P(), P(None, "dp")
    out_m = P("rep", "dp")
    return jax.shard_map(
        body,
        mesh=mesh,
        in_specs=(seq, seq) + (full,) * 3 + (rows,) * 6,
        out_specs=(P("rep"),) * 3 + (out_m,) * 6,
        check_vma=False,
    )
```

```python
import functools

import jax
import jax.numpy as jnp
from jax import lax
from jax.experimental import pallas as pl
from jax.experimental.pallas import tpu as pltpu
from jax.sharding import PartitionSpec as P

f32 = jnp.float32
bf16 = jnp.bfloat16
VMEM_LIMIT = 60 * 1024 * 1024
TN = 256


def params(**kw):
    return pltpu.CompilerParams(vmem_limit_bytes=VMEM_LIMIT, **kw)


def cost(flops, bytes_accessed):
    return pl.CostEstimate(flops=flops, bytes_accessed=bytes_accessed, transcendentals=0)


def sds(shape, dtype):
    return jax.ShapeDtypeStruct(shape, dtype)


NT = (((1,), (1,)), ((), ()))
TNN = (((0,), (0,)), ((), ()))


def mm(a, b):
    return jnp.dot(a, b, preferred_element_type=f32)


def fwd_kernel(rows, x_ref, wg_ref, wu_ref, a_ref, act_ref):
    t = x_ref.shape[0]

    @pl.when(pl.program_id(0) == 0)
    def _():
        for r in range(0, t, rows):
            wide = x_ref[r : r + rows, :].astype(f32)
            scale = lax.rsqrt(jnp.mean(wide * wide, -1, keepdims=True) + 1e-6)
            a_ref[r : r + rows, :] = (wide * scale).astype(bf16)

    for r in range(0, t, rows):
        a = a_ref[r : r + rows, :]
        g = mm(a, wg_ref[...])
        u = mm(a, wu_ref[...])
        act_ref[r : r + rows, :] = (g * jax.nn.sigmoid(g) * u).astype(bf16)


def fwd(x, w_gate, w_up, l):
    t, d = x.shape
    f = w_gate.shape[2]
    whole = pl.BlockSpec((t, d), lambda j: (0, 0))
    wspec = pl.BlockSpec((None, d, TN), lambda j: (l, 0, j))
    tile = pl.BlockSpec((t, TN), lambda j: (0, j))
    return pl.pallas_call(
        functools.partial(fwd_kernel, 512),
        name=f"fwd_gate_up_{l}",
        grid=(f // TN,),
        in_specs=[whole, wspec, wspec],
        out_specs=[whole, tile],
        out_shape=[sds((t, d), bf16), sds((t, f), bf16)],
        compiler_params=params(),
        cost_estimate=cost(4 * t * d * f, 4 * d * f + 2 * t * f + 4 * t * d),
    )(x, w_gate, w_up)


def down_kernel(x_ref, act_ref, w_ref, h_ref, a_ref):
    y = mm(act_ref[...], w_ref[...]).astype(bf16)
    h = (x_ref[...].astype(f32) + y.astype(f32)).astype(bf16)
    h_ref[...] = h
    wide = h.astype(f32)
    scale = lax.rsqrt(jnp.mean(wide * wide, -1, keepdims=True) + 1e-6)
    a_ref[...] = (wide * scale).astype(bf16)


def down(x, act, w_down, l):
    t, d = x.shape
    f = act.shape[1]
    tm = 256
    row = pl.BlockSpec((tm, d), lambda i: (i, 0))
    return pl.pallas_call(
        down_kernel,
        name=f"down_{l}",
        grid=(t // tm,),
        in_specs=[row, pl.BlockSpec((tm, f), lambda i: (i, 0)), pl.BlockSpec((None, f, d), lambda i: (l, 0, 0))],
        out_specs=[row, row],
        out_shape=[sds((t, d), bf16), sds((t, d), bf16)],
        compiler_params=params(),
        cost_estimate=cost(2 * t * d * f, 2 * d * f + 2 * t * f + 6 * t * d),
    )(x, act, w_down)


def silu_back(g, u, dact):
    s = jax.nn.sigmoid(g)
    gs = g * s
    dgate = dact * u * (s + gs * (1.0 - s))
    return dgate.astype(bf16), (dact * gs).astype(bf16)


PAIRED, FOLDED, FINAL, SPREAD, ACROSS, DONE = 1, 2, 3, 4, 5, 6
SLOTS = 4


class Stream:
    def __init__(self, chips, tiles, refs, full, g_ref, state, at_place):
        self.out, self.keep, self.got, self.across, self.near, self.own = refs[:6]
        self.from_near, self.from_far, self.fresh, self.psem, self.sem1, self.sem2, self.gsem, self.lsem = refs[6:]
        self.chips, self.tiles, self.full, self.g_ref, self.state, self.at_place = chips, tiles, full, g_ref, state, at_place
        self.r = self.own.shape[2]
        self.half = self.r // 2
        me = lax.axis_index("dp")
        n = 2 * chips
        self.chip, self.core = me // 2, lax.rem(me, 2)
        self.partner = self.chip * 2 + 1 - self.core
        self.sides = (lax.rem(me + 2, n), lax.rem(me + n - 2, n))
        self.step = pl.program_id(0)

    @staticmethod
    def scratch(chips, s, r, c):
        dma = pltpu.SemaphoreType.DMA
        return [
            pltpu.VMEM((2, chips, s, r, c), bf16),
            pltpu.VMEM((2, chips, s, r, c), bf16),
            pltpu.VMEM((2, chips, s, r, c), bf16),
            pltpu.VMEM((SLOTS, 2, s, r // 2, c), bf16),
            pltpu.VMEM((SLOTS, 2, s, r, c), bf16),
            pltpu.VMEM((SLOTS, s, r, c), bf16),
            pltpu.VMEM((SLOTS, 2, s, r, c), bf16),
            pltpu.VMEM((SLOTS, 2, s, r // 2, c), bf16),
            pltpu.VMEM((SLOTS, s, r, c), bf16),
            dma((2, 2)),
            dma((2, 2, SLOTS)),
            dma((2, 2, SLOTS)),
            dma((8, 2, SLOTS)),
            dma((SLOTS,)),
        ]

    def greet(self):
        barrier = pltpu.get_barrier_semaphore()
        for to in (self.partner, *self.sides):
            pl.semaphore_signal(barrier, inc=1, device_id={"dp": to}, device_id_type=pl.DeviceIdType.MESH)
        pl.semaphore_wait(barrier, 3)

    def remote(self, src, dst, sems, slot, to):
        return pltpu.make_async_remote_copy(
            src_ref=src,
            dst_ref=dst,
            send_sem=sems.at[0, slot],
            recv_sem=sems.at[1, slot],
            device_id={"dp": to},
            device_id_type=pl.DeviceIdType.MESH,
        )

    def pair_copy(self, pair):
        return self.remote(self.out.at[pair], self.got.at[pair], self.psem, pair, self.partner)

    def first(self, slot, at):
        return [
            self.remote(self.across.at[slot, i], self.from_far.at[slot, i], self.sem1.at[i], slot, to) for i, to in enumerate(self.sides)
        ]

    def second(self, slot, at):
        return [self.remote(self.near.at[slot, i], self.from_near.at[slot, i], self.sem2.at[i], slot, to) for i, to in enumerate(self.sides)]

    def place(self, hop, at, lo=0, hi=None):
        return self.at_place(self.full, lax.rem(self.chip + hop, self.chips), self.core, at, lo, self.r if hi is None else hi)

    def gather_1(self, slot, at):
        here, new = self.place(0, at), self.fresh.at[slot]
        ways = [self.remote(new, here, self.gsem.at[i], slot, to) for i, to in enumerate((*self.sides, self.partner))]
        return [*ways, pltpu.make_async_copy(new, here, self.lsem.at[slot])]

    def gather_2(self, slot, at):
        last, half = self.chips - 1, self.half
        before, ahead = self.place(last, at), self.place(1, at)
        low, high = self.place(last, at, 0, half), self.place(1, at, half, self.r)
        ways = ((low, self.sides[0]), (high, self.sides[1]), (before, self.partner), (ahead, self.partner))
        return [self.remote(ref, ref, self.gsem.at[3 + i], slot, to) for i, (ref, to) in enumerate(ways)]

    def gather_3(self, slot, at):
        far = self.place(self.chips // 2, at)
        return [self.remote(far, far, self.gsem.at[7], slot, self.partner)]

    def stage(self, lag):
        at = self.step - lag
        return (at >= 0) & (at < self.tiles), at, lax.rem(jnp.maximum(at, 0), SLOTS)

    def each(self, what, *stages):
        for lag, copies in stages:
            on, at, slot = self.stage(lag)

            @pl.when(on)
            def _():
                for cp in copies(slot, at):
                    getattr(cp, what)()

    def reduce(self):
        half = self.half

        def add(x, y):
            return (x.astype(f32) + y.astype(f32)).astype(bf16)

        on, at, slot = self.stage(FINAL)

        @pl.when(on)
        def _():
            for cp in self.second(slot, at):
                cp.wait()
            total = self.own[slot].astype(f32) + self.from_near[slot, 0].astype(f32) + self.from_near[slot, 1].astype(f32)
            total = total.astype(bf16)
            self.g_ref[...] = total
            for i, (w_ref, m_ref, v_ref) in enumerate(self.state):
                g = total[i].astype(f32)
                m = 0.9 * m_ref[...] + 0.1 * g
                v = 0.95 * v_ref[...] + 0.05 * g * g
                w = w_ref[...].astype(f32)
                self.fresh[slot, i] = (w - 0.02 * (m * lax.rsqrt(v + 1e-8) + 0.1 * w)).astype(bf16)

        on, at, slot = self.stage(FOLDED)

        @pl.when(on)
        def _():
            for cp in self.first(slot, at):
                cp.wait()
            self.near[slot, 0, :, :half] = add(self.near[slot, 0, :, :half], self.from_far[slot, 0])
            self.near[slot, 1, :, half:] = add(self.near[slot, 1, :, half:], self.from_far[slot, 1])

        on, at, slot = self.stage(PAIRED)

        @pl.when(on)
        def _():
            pair = lax.rem(at, 2)
            self.pair_copy(pair).wait()

            def total(hop):
                i = lax.rem(self.chip + hop, self.chips)
                return add(self.keep[pair, i], self.got[pair, i])

            far = total(self.chips // 2)
            self.across[slot, 0] = far[:, :half]
            self.across[slot, 1] = far[:, half:]
            self.near[slot, 0] = total(1)
            self.near[slot, 1] = total(self.chips - 1)
            self.own[slot] = total(0)

        self.each("start", (PAIRED, self.first), (FOLDED, self.second), (FINAL, self.gather_1))

    def gather(self):
        self.each("wait", (DONE, self.gather_3), (ACROSS, self.gather_2), (SPREAD, self.gather_1))
        self.each("start", (SPREAD, self.gather_2), (ACROSS, self.gather_3))

        @pl.when(self.step < self.tiles)
        def _():
            self.pair_copy(lax.rem(self.step, 2)).start()


def grads_kernel(chips, tiles, wanted, *refs):
    a_ref, dy_ref, p_ref, q_ref, wd_ref = refs[:5]
    state = (refs[5:8], refs[8:11])
    refs = refs[11:]
    if wanted:
        (h_ref, dh_ref), refs = (refs[0], refs[1]), refs[2:]
        da_ref, refs = refs[3], refs[:3] + refs[4:]
    down_ref, g_ref, full, dg_ref, du_ref, at_ref, act_ref = refs[:7]
    t, d = a_ref.shape
    r = d // (2 * chips)

    def at_place(full, x, core, at, lo, hi):
        return full.at[:, x, core, pl.ds(lo, hi - lo), pl.ds(pl.multiple_of(at * TN, TN), TN)]

    group = Stream(chips, tiles, refs[7:], full, g_ref, state, at_place)
    step, core = group.step, group.core

    @pl.when(step == 0)
    def _():
        group.greet()
        if wanted:
            da_ref[...] = jnp.zeros_like(da_ref)
        for part, which in enumerate((1 - core, core)):
            for x in range(chips):
                at = pl.multiple_of((2 * x + which) * r, 128)
                to = (part * chips + x) * r
                at_ref[to : to + r, :] = a_ref[:, pl.ds(at, r)].T

    @pl.when(step < tiles)
    def _():
        rows = 512
        for lo in range(0, t, rows):
            at = slice(lo, lo + rows)
            g, u = mm(a_ref[at, :], p_ref[...]), mm(a_ref[at, :], q_ref[...])
            dact = lax.dot_general(dy_ref[at, :], wd_ref[...], NT, preferred_element_type=f32)
            act_ref[at, :] = (g * jax.nn.sigmoid(g) * u).astype(bf16)
            dg_ref[at, :], du_ref[at, :] = silu_back(g, u, dact.astype(bf16).astype(f32))

    group.reduce()

    if wanted:
        rows = 512

        @pl.when(step < tiles)
        def _():
            for lo in range(0, t, rows):
                at = slice(lo, lo + rows)
                term = lax.dot_general(dg_ref[at, :], p_ref[...], NT, preferred_element_type=f32)
                da_ref[at, :] += term + lax.dot_general(du_ref[at, :], q_ref[...], NT, preferred_element_type=f32)

        @pl.when(step == tiles)
        def _():
            for lo in range(0, t, rows):
                at = slice(lo, lo + rows)
                da = da_ref[at, :].astype(bf16).astype(f32)
                wide = h_ref[at, :].astype(f32)
                scale = lax.rsqrt(jnp.mean(wide * wide, -1, keepdims=True) + 1e-6)
                norm = wide * scale
                back_ = scale * (da - norm * jnp.mean(da * norm, -1, keepdims=True))
                dh_ref[at, :] = (dy_ref[at, :].astype(f32) + back_.astype(bf16).astype(f32)).astype(bf16)

    @pl.when(step < tiles)
    def _():
        pair = lax.rem(step, 2)
        for s, ref in enumerate((dg_ref, du_ref)):
            for part, to in ((0, group.out), (1, group.keep)):
                term = mm(at_ref[part * (d // 2) : (part + 1) * (d // 2), :], ref[...]).astype(bf16)
                for x in range(chips):
                    to[pair, x, s] = term[x * r : (x + 1) * r]
        down_ref[...] = lax.dot_general(act_ref[...], dy_ref[...], TNN, preferred_element_type=f32).astype(bf16)

    group.gather()


def grads(a, dy, w_gate, w_up, w_down, state, h, l, chips, name):
    wanted = h is not None
    t, d = a.shape
    f = w_down.shape[1]
    tiles = f // TN
    r = d // (2 * chips)
    whole = pl.BlockSpec((t, d), lambda j: (0, 0), pipeline_mode=pl.Buffered(1))

    def at(j):
        return jnp.minimum(j, tiles - 1)

    wspec = pl.BlockSpec((None, d, TN), lambda j: (l, 0, at(j)))
    dspec = pl.BlockSpec((None, TN, d), lambda j: (l, at(j), 0))

    def late(j):
        return jnp.clip(j - FINAL, 0, tiles - 1)

    sspec = pl.BlockSpec((None, r, TN), lambda j: (l, 0, late(j)))
    mine = pl.BlockSpec((None, r, TN), lambda j: (l, lax.axis_index("dp"), late(j)))
    out_specs = [pl.BlockSpec((TN, d), lambda j: (at(j), 0)), pl.BlockSpec((2, r, TN), lambda j: (0, 0, late(j)))]
    out_specs.append(pl.BlockSpec(memory_space=pl.ANY))
    out_shape = [sds((f, d), bf16), sds((2, r, f), bf16), sds((2, chips, 2, r, f), bf16)]
    scratch = [pltpu.VMEM((t, TN), bf16)] * 2
    more = []
    if wanted:
        out_specs, out_shape, more = [pl.BlockSpec((t, d), lambda j: (0, 0))] + out_specs, [sds((t, d), bf16)] + out_shape, [h]
        scratch = [pltpu.VMEM((t, d), f32)] + scratch
    scratch += [pltpu.VMEM((d, t), bf16), pltpu.VMEM((t, TN), bf16)] + Stream.scratch(chips, 2, r, TN)
    return pl.pallas_call(
        functools.partial(grads_kernel, chips, tiles, wanted),
        name=f"grads_{name}",
        grid=(tiles + DONE,),
        in_specs=[whole, whole, wspec, wspec, dspec] + [mine, sspec, sspec] * 2 + [whole] * len(more),
        out_specs=out_specs,
        out_shape=out_shape,
        scratch_shapes=scratch,
        compiler_params=params(collective_id=l, has_side_effects=True),
        cost_estimate=cost(12 * t * d * f, 20 * t * f),
    )(a, dy, w_gate, w_up, w_down, *state, *more)


def width(c):
    return c // 2 if c % 256 == 0 else c


def pair_kernel(chips, got_ref, keep_ref, across_a, across_b, right, left, own):
    me = lax.axis_index("dp")
    chip, core = me // 2, lax.rem(me, 2)
    half = got_ref.shape[1] // 2

    def total(hop):
        i = lax.rem(chip + hop, chips)
        mine = keep_ref[i, core] if len(keep_ref.shape) == 4 else keep_ref[i]
        return (mine.astype(f32) + got_ref[i].astype(f32)).astype(bf16)

    across = total(2)
    across_a[...] = across[:half]
    across_b[...] = across[half:]
    right[...] = total(1)
    left[...] = total(3)
    own[...] = total(0)


def pair_add(got, keep, name):
    s, chips, r, c = got.shape
    tc = width(c)
    whole = pl.BlockSpec((None, chips, r, tc), lambda i, j: (i, 0, 0, j))
    wide = pl.BlockSpec((None, chips, 2, r, tc), lambda i, j: (i, 0, 0, 0, j)) if keep.ndim == 5 else whole
    one = pl.BlockSpec((None, r, tc), lambda i, j: (i, 0, j))
    half = pl.BlockSpec((None, r // 2, tc), lambda i, j: (i, 0, j))
    return pl.pallas_call(
        functools.partial(pair_kernel, chips),
        name=f"pair_add_{name}",
        grid=(s, c // tc),
        in_specs=[whole, wide],
        out_specs=[half, half, one, one, one],
        out_shape=[sds((s, r // 2, c), bf16)] * 2 + [sds((s, r, c), bf16)] * 3,
        compiler_params=params(),
        cost_estimate=cost(16 * s * r * c, 24 * s * r * c),
    )(got, keep)


def fold_kernel(right, left, a, b, right_out, left_out):
    right_out[...] = (right[...].astype(f32) + a[...].astype(f32)).astype(bf16)
    left_out[...] = (left[...].astype(f32) + b[...].astype(f32)).astype(bf16)


def fold(right, left, a, b, name):
    s, r, c = right.shape
    tc = width(c)
    lo = pl.BlockSpec((None, r // 2, tc), lambda i, j: (i, 0, j))
    hi = pl.BlockSpec((None, r // 2, tc), lambda i, j: (i, 1, j))
    return pl.pallas_call(
        fold_kernel,
        name=f"fold_{name}",
        grid=(s, c // tc),
        in_specs=[lo, hi, lo, lo],
        out_specs=[lo, hi],
        out_shape=[sds((s, r, c), bf16)] * 2,
        input_output_aliases={0: 0, 1: 1},
        compiler_params=params(),
        cost_estimate=cost(4 * s * r * c, 6 * s * r * c),
    )(right, left, a, b)


def adamw_kernel(n, *refs):
    sums, (w_ref, m_ref, v_ref), (nw_ref, nm_ref, nv_ref) = refs[:n], refs[n : n + 3], refs[-3:]
    g = sums[0][...].astype(f32)
    for other in sums[1:]:
        g = g + other[...].astype(f32)
    g = g.astype(bf16).astype(f32)
    m = 0.9 * m_ref[...] + 0.1 * g
    v = 0.95 * v_ref[...] + 0.05 * g * g
    w = w_ref[...].astype(f32)
    nm_ref[...] = m
    nv_ref[...] = v
    nw_ref[...] = (w - 0.02 * (m * lax.rsqrt(v + 1e-8) + 0.1 * w)).astype(bf16)


def adamw(sums, s, w, m, v, l, col, moments, new, name):
    n, r, c = sums[0].shape
    tr, tc = r // 2, TN if col or c < m.shape[2] else width(c)
    part = pl.BlockSpec((None, tr, tc), lambda i, j: (s, i, j))
    block = pl.BlockSpec((None, tr, tc), lambda i, j: (l, i, j + col // tc))
    mine = pl.BlockSpec((None, tr, tc), lambda i, j: (l, lax.axis_index("dp") * (r // tr) + i, j + col // tc))
    anyspec = pl.BlockSpec(memory_space=pl.ANY)
    more, alias = [], {}
    for at, t in ((0, new),) + ((1, None), (2, None)) if moments is None else ((0, new), (1, moments[0]), (2, moments[1])):
        if t is not None:
            alias[len(sums) + 3 + len(more)] = at
            more.append(t)
    return pl.pallas_call(
        functools.partial(adamw_kernel, len(sums)),
        name=f"adamw_{name}",
        grid=(r // tr, c // tc),
        in_specs=[part] * len(sums) + [mine, block, block] + [anyspec] * len(more),
        out_specs=[part, block, block],
        out_shape=[sds((n, r, c), bf16), sds(m.shape, f32), sds(v.shape, f32)],
        input_output_aliases=alias,
        compiler_params=params(),
        cost_estimate=cost(20 * r * c, 30 * r * c),
    )(*sums, w, m, v, *more)


def moments_kernel(g_ref, m_ref, v_ref, *rest):
    nm_ref, nv_ref = rest[-2:]
    g = g_ref[...].astype(f32)
    nm_ref[...] = 0.9 * m_ref[...] + 0.1 * g
    nv_ref[...] = 0.95 * v_ref[...] + 0.05 * g * g


def new_moments(g, s, m, v, l, into, name):
    _, r, c = g.shape
    tr, tc = r // 2, width(c)
    part = pl.BlockSpec((None, tr, tc), lambda i, j: (s, i, j))
    block = pl.BlockSpec((None, tr, tc), lambda i, j: (l, i, j))
    more = [] if into is None else list(into)
    return pl.pallas_call(
        moments_kernel,
        name=f"moments_{name}",
        grid=(r // tr, c // tc),
        in_specs=[part, block, block] + [pl.BlockSpec(memory_space=pl.ANY)] * len(more),
        out_specs=[block, block],
        out_shape=[sds(m.shape, f32), sds(v.shape, f32)],
        input_output_aliases={3: 0, 4: 1} if more else {},
        compiler_params=params(),
        cost_estimate=cost(10 * r * c, 18 * r * c),
    )(g, m, v, *more)


def stack_kernel(k, full_ref, *rest):
    for s, out in enumerate(rest[-k:]):
        out[...] = full_ref[s]


def stack_layer(full, layers, l, into, name):
    k, d, f = full.shape
    tr = d // 8
    more = [t for t in into if t is not None]
    block = pl.BlockSpec((None, tr, f), lambda i: (l, i, 0))
    return pl.pallas_call(
        functools.partial(stack_kernel, k),
        name=f"stack_{name}",
        grid=(d // tr,),
        in_specs=[pl.BlockSpec((k, tr, f), lambda i: (0, i, 0))] + [pl.BlockSpec(memory_space=pl.ANY)] * len(more),
        out_specs=[block] * k,
        out_shape=[sds((layers, d, f), bf16)] * k,
        input_output_aliases={1 + i: i for i in range(len(more))},
        compiler_params=params(),
        cost_estimate=cost(k * d * f, 4 * k * d * f),
    )(full, *more)


def place_kernel(l, col, chips, kinds, n, k, *refs):
    pieces = refs[:n]
    refs = refs[n:]
    bufs, (isem, osem) = refs[-n - 2 : -2], refs[-2:]
    outs = refs[-n - 2 - k : -n - 2]
    me = lax.axis_index("dp")
    x, core = me // 2, lax.rem(me, 2)
    ins = []
    for i in range(n):
        cp = pltpu.make_async_copy(pieces[i], bufs[i], isem.at[i])
        cp.start()
        ins.append(cp)
    going = []
    for i, (hop, other, lo, hi) in enumerate(kinds):
        ins[i].wait()
        xi = lax.rem(x + hop, chips)
        ci = 1 - core if other else core
        for s, out in enumerate(outs):
            dst = out.at[l, xi, ci, pl.ds(lo, hi - lo), pl.ds(col, pieces[i].shape[2])]
            cp = pltpu.make_async_copy(bufs[i].at[s], dst, osem.at[i, s])
            cp.start()
            going.append(cp)
    for cp in going:
        cp.wait()


def place(pieces, kinds, shapes, l, col, into, chips, name):
    n, k = len(pieces), len(shapes)
    into = [t for t in into if t is not None]
    anyspec = pl.BlockSpec(memory_space=pl.ANY)
    moved = sum(p.size for p in pieces)
    return pl.pallas_call(
        functools.partial(place_kernel, l, col, chips, tuple(kinds), n, k),
        name=f"place_{name}",
        in_specs=[anyspec] * (n + len(into)),
        out_specs=[anyspec] * k,
        out_shape=[sds(shape, bf16) for shape in shapes],
        scratch_shapes=[pltpu.VMEM(p.shape, bf16) for p in pieces] + [pltpu.SemaphoreType.DMA((n,)), pltpu.SemaphoreType.DMA((n, k))],
        input_output_aliases={n + i: i for i in range(len(into))},
        compiler_params=params(),
        cost_estimate=cost(moved, 4 * moved),
    )(*pieces, *into)


def solution(mesh):
    n = mesh.shape["dp"]
    chips = n // 2
    PAIR = [(i, i ^ 1) for i in range(n)]
    RIGHT = [(i, (i + 2) % n) for i in range(n)]
    LEFT = [(i, (i - 2) % n) for i in range(n)]

    def send(t, way):
        return lax.ppermute(t, "dp", way)

    def body(x, dy, w_gate, w_up, w_down, m_gate, m_up, m_down, v_gate, v_up, v_down):
        me = lax.axis_index("dp")
        core = me % 2
        x, dy = x[0], dy[0]
        layers, d, f = w_gate.shape
        tiles = f // TN

        own_w = {"gate": w_gate, "up": w_up, "down": w_down}
        m_in = {"gate": m_gate, "up": m_up, "down": m_down}
        v_in = {"gate": v_gate, "up": v_up, "down": v_down}
        moments, new_w = {}, {}

        class Unit:
            def __init__(self, keys, l, col, name, out=None, keep=None, total=None):
                self.keep, self.keys, self.l, self.col, self.name = keep, keys, l, col, name
                self.stage, self.hold = 0, None
                if total is None:
                    self.flight = [send(out, PAIR)]
                else:
                    self.own, self.flight, self.stage = total, [], 2
                    self.advance()

            def advance(self):
                getattr(self, ("reduce_1", "reduce_2", "step", "gather_2", "gather_3", "finish")[self.stage])()
                self.stage += 1

            def reduce_1(self):
                a, b, self.right, self.left, self.own = pair_add(self.flight[0], self.keep, self.name)
                if self.hold is not None:
                    a, b, self.hold = lax.optimization_barrier((a, b, self.hold))
                self.flight = [send(a, RIGHT), send(b, LEFT)]

            def reduce_2(self):
                right, left = fold(self.right, self.left, *self.flight, self.name)
                if self.hold is not None:
                    right, left, self.hold = lax.optimization_barrier((right, left, self.hold))
                self.flight = [send(right, RIGHT), send(left, LEFT)]

            def step(self):
                w = None
                sums = [self.own, *self.flight]
                for s, key in enumerate(self.keys):
                    w, *moments[key] = adamw(
                        sums, s, own_w[key], m_in[key], v_in[key], self.l, self.col, moments.get(key), w, f"{self.name}_{key}"
                    )
                self.w = w
                self.flight = [send(w, RIGHT), send(w, LEFT), send(w, PAIR)]

            def gather_2(self):
                wl, wr, pw = self.flight
                half = wl.shape[1] // 2
                self.pieces = [self.w, wl, wr, pw]
                self.flight = [send(wl[:, :half], RIGHT), send(wr[:, half:], LEFT), send(wl, PAIR), send(wr, PAIR)]

            def gather_3(self):
                o1, o2, pwl, pwr = self.flight
                self.pieces += [pwl, pwr, o1, o2]
                self.flight = [send(o1, PAIR), send(o2, PAIR)]

            def finish(self):
                pieces = self.pieces + self.flight
                r = self.w.shape[1]
                half = r // 2
                kinds = [(0, False, 0, r), (3, False, 0, r), (1, False, 0, r), (0, True, 0, r), (3, True, 0, r), (1, True, 0, r)]
                kinds += [(2, o, lo, hi) for o in (False, True) for lo, hi in ((0, half), (half, r))]
                shapes = [(layers, chips, 2, r, own_w[key].shape[2]) for key in self.keys]
                into = [None if key not in new_w else new_w[key].reshape(shape) for key, shape in zip(self.keys, shapes)]
                for key, t in zip(self.keys, place(pieces, kinds, shapes, self.l, self.col, into, chips, self.name)):
                    new_w[key] = t

        def after(units, *inputs):
            inputs, flights = lax.optimization_barrier((inputs, [u.flight for u in units]))
            for u, flight in zip(units, flights):
                u.flight = flight
                u.advance()
            return inputs

        def down_unit(g, l):
            g = g.reshape(1, chips, 2, f // n, d)
            out = lax.dynamic_index_in_dim(g, 1 - core, 2, keepdims=False)
            return Unit(("down",), l, 0, f"{l}d", out, g)

        kept = []
        h = x
        for l in range(layers - 1):
            a, act = fwd(h, w_gate, w_up, l)
            kept.append((h, a))
            h, a = down(h, act, w_down, l)
        l = layers - 1
        def state_of(*keys):
            return [t[k] for k in keys for t in (own_w, m_in, v_in)]

        def moments_of(g, i, key, l):
            moments[key] = new_moments(g, i, m_in[key], v_in[key], l, moments.get(key), f"{l}_{key}")

        def stack_of(full, keys, l):
            full = full.reshape(len(keys), -1, full.shape[-1])
            for key, t in zip(keys, stack_layer(full, layers, l, [new_w.get(k) for k in keys], f"{l}_{keys[-1]}")):
                new_w[key] = t

        def beside(unit, *work):
            for f_, *args in work:
                f_(*args)
            made = [{k: v for k, v in vars(u).items() if k in ("own", "w")} for u in live]
            unit.flight, moments_, new_w_, made = lax.optimization_barrier((unit.flight, dict(moments), dict(new_w), made))
            moments.update(moments_)
            new_w.update(new_w_)
            for u, values in zip(live, made):
                vars(u).update(values)
            unit.advance()

        both = ("gate", "up")
        jobs, units, live = [], [], []
        for l in range(layers - 1, -1, -1):
            if units:
                units[-1].hold = dy
                beside(units[-1])
                dy, units[-1].hold = units[-1].hold, None
            *cot, g_down, g, full = grads(a, dy, w_gate, w_up, w_down, state_of(*both), h if l else None, l, chips, f"{l}")
            jobs += [(moments_of, g, i, key, l) for i, key in enumerate(both)] + [(stack_of, full, both, l)]
            if l:
                dy = cot[0]
                h, a = kept[l - 1]
                units.append(down_unit(g_down, l))
                live.append(units[-1])
        (unit,) = units
        unit.hold = g_down
        beside(unit)
        tail = down_unit(unit.hold, 0)
        unit.hold = None
        live.append(tail)
        beside(tail)
        beside(tail, jobs[0], jobs[3], jobs[4])
        beside(unit)
        beside(tail, jobs[2])
        beside(unit, jobs[1])
        beside(tail, jobs[5])
        beside(unit)
        unit.advance()
        beside(tail)
        while tail.stage < 6:
            tail.advance()
        keys = ("gate", "up", "down")
        ws = tuple(new_w[k].reshape(w.shape) for k, w in zip(keys, (w_gate, w_up, w_down)))
        return ws + tuple(moments[k][0] for k in keys) + tuple(moments[k][1] for k in keys)

    seq, full, rows = P(("rep", "dp")), P(), P(None, "dp")
    out_m = P("rep", "dp")
    return jax.shard_map(
        body,
        mesh=mesh,
        in_specs=(seq, seq) + (full,) * 3 + (rows,) * 6,
        out_specs=(P("rep"),) * 3 + (out_m,) * 6,
        check_vma=False,
    )
```
